32 devices in a mesh: lon: 8 (over z, x), ch: 4 (over y, core).
Axes of the slice: x: 2, y: 2, z: 4, core: 2. Of those that a mesh axis runs over, the one named last changes fastest.
Arguments:
- grid_inputs: bfloat16 [230400, 474], P('lon'), may hold values from -6 to 6
- embed_weight: bfloat16 [474, 512], replicated, may hold values from -0.25 to 0.25
- embed_bias: float32 [512], replicated, may hold values from -3 to 3
- mesh_latent: bfloat16 [5120, 512], P('lon', 'ch'), may hold values from -6 to 6
- edge_features: bfloat16 [4, 180224], P(None, 'lon'), may hold values from -6 to 6
- senders: int32 [180224], P('lon'), may hold values from 0 to 230399, as said below
- receivers: int32 [180224], P('lon'), may hold values from 0 to 5119, as said below
- sender_weight: bfloat16 [512, 512], P(None, 'ch'), may hold values from -0.25 to 0.25
- receiver_weight: bfloat16 [512, 512], P(None, 'ch'), may hold values from -0.25 to 0.25
- feature_weight: bfloat16 [4, 512], P(None, 'ch'), may hold values from -3 to 3
- hidden_bias: float32 [512], P('ch'), may hold values from -3 to 3
- message_weight: bfloat16 [512, 512], P('ch'), may hold values from -0.25 to 0.25
- message_bias: float32 [512], replicated, may hold values from -1.2 to 1.2
- norm_gain: float32 [512], P('ch'), may hold values from 0.5 to 1.5
- norm_shift: float32 [512], P('ch'), may hold values from -3 to 3
Outputs:
- mesh_out: bfloat16 [5120, 512], P('lon', 'ch')
The draws below stay inside these ranges and needn't reach their ends.
Inputs may be any that keep to these rules, and one draw needn't show every extreme that they name: Edge e belongs to block b = e // 22528. Its sender is c * 640 + t with latitude row t and a column c that lies, counted around the closed circle of 360 columns, at most 4 columns before or after the block's own columns b * 45 to b * 45 + 44; some block reaches 4 columns on both sides. Within each aligned run of min(2048, 22528) edges of a block, the senders' columns, counted from the block's first widened column, lie within 7 consecutive columns. `receivers`: the receiver of edge e lies among the mesh nodes b * 640 to b * 640 + 639 of its block b = e // 22528; a mesh node may receive no edge.
All inputs are finite; a program needn't handle non-finite values.
Results may differ from the reference program's by a relative error of at most 0.0028.
Values may be sent and summed in bfloat16 or wider, within the bound.
A program may use at most 128 MiB of HBM per device.

```python
import jax
import jax.numpy as jnp
from jax import lax

CIN = 474
L = 512
CE = 4
COLS_DEV = 45
LAT = 640
M_DEV = 640
E_DEV = 22528
HALO = 4
NCOL = 360
NGRID = 230400
NMESH = 5120
NEDGE = 180224


def draw_senders(key, part):
    base_key = jax.random.fold_in(key, 11)
    reach_key, pick_key, col_key, lat_key = jax.random.split(base_key, 4)
    blocks = NEDGE // E_DEV
    reaches = jax.random.randint(reach_key, (blocks,), 1, HALO + 1)
    chosen = jax.random.randint(pick_key, (), 0, blocks)
    reaches = jnp.where(jnp.arange(blocks) == chosen, HALO, reaches)
    edge_ids = jnp.arange(NEDGE)
    owning = edge_ids // E_DEV
    within = edge_ids % E_DEV
    reach = reaches[owning]
    span = COLS_DEV + 2 * reach
    jitter = jax.random.randint(col_key, (NEDGE,), 0, 2)
    offset = jnp.minimum(within * span // E_DEV + jitter, span - 1)
    offset = jnp.where(within == 0, 0, offset)
    offset = jnp.where(within == E_DEV - 1, span - 1, offset)
    column = jnp.mod(owning * COLS_DEV + offset - reach, NCOL)
    latitude = jax.random.randint(lat_key, (NEDGE,), 0, LAT)
    return (column * LAT + latitude).astype(jnp.int32)


def draw_receivers(key, part):
    base_key = jax.random.fold_in(key, 23)
    edge_ids = jnp.arange(NEDGE)
    slots = jax.random.randint(base_key, (NEDGE,), 0, M_DEV)
    return (edge_ids // E_DEV * M_DEV + slots).astype(jnp.int32)


def shard_levels(key, extent, cuts, smallest, high):
    def one(axis_at, parts):
        steps = jax.random.uniform(jax.random.fold_in(jax.random.fold_in(key, 6), axis_at), (parts,), jnp.float32, smallest / len(cuts), high / len(cuts))
        return jnp.repeat(jnp.exp(steps), extent[axis_at] // parts).reshape((-1,) + (1,) * (len(extent) - axis_at - 1))

    level = one(*cuts[0])
    for cut in cuts[1:]:
        level = level * one(*cut)
    return level


def normal_values(own_key, shape, scale, bound, shards=(), held_as=jnp.bfloat16):
    result = scale * jax.random.normal(own_key, shape, jnp.float32)
    if shards:
        result = result * shard_levels(own_key, shape, shards, -0.22, 0.18)
    return jnp.clip(result, -bound, bound).astype(held_as)


def setup_inputs(seed: int = 0) -> dict:
    keys = jax.random.split(jax.random.key(seed), 16)
    grid_inputs = normal_values(keys[0], (NGRID, CIN), 1.0, 6.0, ((0, 8),))
    embed_weight = normal_values(keys[1], (CIN, L), CIN ** -0.5, 0.25)
    embed_bias = normal_values(keys[2], (L,), 0.5, 3.0, (), jnp.float32)
    mesh_latent = normal_values(keys[3], (NMESH, L), 1.0, 6.0, ((0, 8), (1, 4)))
    edge_features = normal_values(keys[4], (CE, NEDGE), 1.0, 6.0, ((1, 8),))
    senders = draw_senders(jax.random.fold_in(keys[15], 71), 0)
    receivers = draw_receivers(jax.random.fold_in(keys[15], 71), 0)
    sender_weight = normal_values(keys[7], (L, L), L ** -0.5, 0.25, ((1, 4),))
    receiver_weight = normal_values(keys[8], (L, L), L ** -0.5, 0.25, ((1, 4),))
    feature_weight = normal_values(keys[9], (CE, L), CE ** -0.5, 3.0, ((1, 4),))
    hidden_bias = normal_values(keys[10], (L,), 0.5, 3.0, ((0, 4),), jnp.float32)
    message_weight = normal_values(keys[11], (L, L), L ** -0.5, 0.25, ((0, 4),))
    message_bias = normal_values(keys[12], (L,), 0.2, 1.2, (), jnp.float32)
    norm_gain = jnp.clip(1.0 + 0.1 * jax.random.normal(keys[13], (L,), jnp.float32), 0.5, 1.5)
    norm_shift = normal_values(keys[14], (L,), 0.5, 3.0, ((0, 4),), jnp.float32)
    return {"grid_inputs": grid_inputs, "embed_weight": embed_weight, "embed_bias": embed_bias, "mesh_latent": mesh_latent, "edge_features": edge_features, "senders": senders, "receivers": receivers, "sender_weight": sender_weight, "receiver_weight": receiver_weight, "feature_weight": feature_weight, "hidden_bias": hidden_bias, "message_weight": message_weight, "message_bias": message_bias, "norm_gain": norm_gain, "norm_shift": norm_shift}


def reference(grid_inputs, embed_weight, embed_bias, mesh_latent, edge_features, senders, receivers, sender_weight, receiver_weight, feature_weight, hidden_bias, message_weight, message_bias, norm_gain, norm_shift):
    latent = jax.nn.silu(jnp.dot(grid_inputs, embed_weight, preferred_element_type=jnp.float32) + embed_bias).astype(jnp.bfloat16)
    sent_terms = jnp.dot(latent, sender_weight, preferred_element_type=jnp.float32)
    recv_terms = jnp.dot(mesh_latent, receiver_weight, preferred_element_type=jnp.float32)
    blocks = NEDGE // E_DEV
    feature_blocks = jnp.transpose(edge_features.reshape(CE, blocks, E_DEV), (1, 2, 0))
    send_blocks = senders.reshape(blocks, E_DEV)
    recv_blocks = receivers.reshape(blocks, E_DEV)

    def accumulate(carried, pieces):
        totals, tallies = carried
        send_ids, recv_ids, features = pieces
        before = sent_terms[send_ids] + recv_terms[recv_ids]
        before = before + jnp.dot(features, feature_weight, preferred_element_type=jnp.float32) + hidden_bias
        hidden = jax.nn.silu(before).astype(jnp.bfloat16)
        totals = totals + jax.ops.segment_sum(hidden.astype(jnp.float32), recv_ids, num_segments=NMESH)
        tallies = tallies + jax.ops.segment_sum(jnp.ones((E_DEV,), jnp.float32), recv_ids, num_segments=NMESH)
        return ((totals, tallies), None)
    start = (jnp.zeros((NMESH, L), jnp.float32), jnp.zeros((NMESH,), jnp.float32))
    (totals, tallies), ignored = lax.scan(accumulate, start, (send_blocks, recv_blocks, feature_blocks))
    aggregated = jnp.dot(totals, message_weight.astype(jnp.float32), precision=lax.Precision.HIGHEST)
    aggregated = aggregated + tallies[:, None] * message_bias
    centre = lax.optimization_barrier(jnp.mean(aggregated, axis=1, keepdims=True))
    spread = lax.optimization_barrier(jnp.mean(jnp.square(aggregated - centre), axis=1, keepdims=True))
    normed = (aggregated - centre) * lax.rsqrt(spread + 1.0)
    return (mesh_latent.astype(jnp.float32) + normed * norm_gain + norm_shift).astype(jnp.bfloat16)
```

```python
import functools

import jax
import jax.numpy as jnp
from jax import lax
from jax.experimental import pallas as pl
from jax.experimental.pallas import tpu as pltpu
from jax.sharding import PartitionSpec as P

LAT = 640
HALO = 4
UNIT = 512
WINDOW = 7
SLOTS = 8
LANES = 128
CHUNK = 256


def silu(v):
    half = 0.5 * v
    return half + half * jnp.tanh(half)


def pick_units(low_ref, high_ref, list_ref, columns, halo_turn):
    me = lax.axis_index("ch")
    ch_count = lax.axis_size("ch")
    units = low_ref.shape[0]
    one = lambda flag: jnp.where(flag, 1, 0)
    at_left = [one(low_ref[u] < HALO) for u in range(units)]
    at_right = [one(high_ref[u] >= HALO + columns) for u in range(units)]
    lefts, rights = sum(at_left), sum(at_right)
    inner_count = units - lefts - rights
    even_share = -(-units // ch_count)
    first = jnp.minimum(jnp.maximum(even_share - lefts, 0), inner_count)
    last = jnp.maximum(inner_count - jnp.maximum(even_share - rights, 0), first)
    middle = lambda k: first + lax.div((last - first) * (k - 1), ch_count - 2)
    begin = jnp.where(me == 0, 0, middle(me))
    end = jnp.where(me == ch_count - 1, inner_count, middle(me + 1))
    count, rank = jnp.int32(0), jnp.int32(0)
    for u in range(units):
        inner = 1 - at_left[u] - at_right[u]
        if halo_turn:
            mine = jnp.where(me == 0, at_left[u], 0) + jnp.where(
                me == ch_count - 1, at_right[u], 0
            )
        else:
            inside = jnp.logical_and(rank >= begin, rank < end)
            mine = jnp.where(inside, inner, 0)
        list_ref[count] = u
        count = count + mine
        rank = rank + inner
    return count


def gather_kernel(
    columns,
    halo_turn,
    low_ref,
    high_ref,
    send_ref,
    x_ref,
    halo_ref,
    embed_ref,
    bias_ref,
    out_ref,
    list_ref,
    events,
    event_at,
    held_column,
    index,
    points,
    table,
    even,
    odd,
    packed,
    index_sem,
    point_sem,
    out_sem,
):
    parts = out_ref.shape[1] // LANES
    unit = send_ref.shape[1]
    step = LAT * parts
    depth = points.shape[0]
    count = pick_units(low_ref, high_ref, list_ref, columns, halo_turn)

    for n in range(SLOTS):
        held_column[n] = -1

    def note_unit(n, total):
        u = list_ref[n]
        event_at[n] = total

        def note(column, total):
            slot = lax.rem(column, SLOTS)
            new = jnp.where(held_column[slot] == column, 0, 1)
            held_column[slot] = column
            events[total] = column
            return total + new

        return lax.fori_loop(low_ref[u], high_ref[u] + 1, note, total)

    total = lax.fori_loop(0, count, note_unit, jnp.int32(0))
    event_at[count] = total

    def fetch(event):
        column, slot = events[event], lax.rem(event, depth)

        def copy(source, place):
            start = pl.multiple_of(place * LAT, LANES)
            return pltpu.make_async_copy(
                source.at[:, pl.ds(start, LAT)], points.at[slot], point_sem.at[slot]
            )

        if not halo_turn:
            copy(x_ref, column - HALO).start()
            return
        last = column >= HALO + columns
        outside = jnp.logical_or(column < HALO, last)
        pl.when(outside)(
            lambda: copy(halo_ref, jnp.where(last, column - HALO - columns, column)).start()
        )
        pl.when(jnp.logical_not(outside))(lambda: copy(x_ref, column - HALO).start())

    def fetch_index(n):
        slot = lax.rem(n, 2)
        return pltpu.make_async_copy(
            send_ref.at[list_ref[n]], index.at[slot], index_sem.at[slot]
        )

    for event in range(depth):
        pl.when(event < total)(functools.partial(fetch, event))
    pl.when(count > 0)(lambda: fetch_index(0).start())

    def one_event(event, carry):
        slot = lax.rem(event, depth)
        pltpu.make_async_copy(
            x_ref.at[:, pl.ds(0, LAT)], points.at[slot], point_sem.at[slot]
        ).wait()
        before = lax.dot_general(
            points[slot], embed_ref[...], (((0,), (0,)), ((), ())),
            preferred_element_type=jnp.float32,
        ) + bias_ref[...]
        latent = silu(before)
        base = lax.rem(events[event], SLOTS) * step
        for j in range(parts):
            table[pl.ds(base + j, LAT, stride=parts), :] = latent[:, j * LANES:(j + 1) * LANES]
        pl.when(event + depth < total)(lambda: fetch(event + depth))
        return carry

    def gather(n, half, held):
        slot = lax.rem(n, 2)
        for i in range(CHUNK):
            place = pl.multiple_of(index[slot, half * CHUNK + i], parts)
            held[pl.ds(parts * i, parts), :] = table[pl.ds(place, parts), :]

    def leave(n, half, held):
        start = pl.multiple_of(list_ref[n] * unit + half * CHUNK, CHUNK)
        for j in range(parts):
            packed[half, :, j * LANES:(j + 1) * LANES] = (
                held[pl.ds(j, CHUNK, stride=parts), :].astype(jnp.bfloat16)
            )
        pltpu.make_async_copy(
            packed.at[half], out_ref.at[pl.ds(start, CHUNK), :], out_sem.at[half]
        ).start()

    def settle(half):
        pltpu.make_async_copy(
            packed.at[half], out_ref.at[pl.ds(0, CHUNK), :], out_sem.at[half]
        ).wait()

    def one_unit(n, carry):
        pl.when(n + 1 < count)(lambda: fetch_index(n + 1).start())
        lax.fori_loop(event_at[n], event_at[n + 1], one_event, 0)
        fetch_index(n).wait()
        for half in range(2):
            pl.when(n > 0)(functools.partial(settle, half))
        leave(jnp.maximum(n - 1, 0), 1, odd)
        gather(n, 0, even)
        leave(n, 0, even)
        gather(n, 1, odd)
        return carry

    lax.fori_loop(0, count, one_unit, 0)

    @pl.when(count > 0)
    def _():
        settle(1)
        leave(count - 1, 1, odd)
        for half in range(2):
            settle(half)


def gathered(low, high, send, points, halo, embed_weight, embed_bias, halo_turn):
    channels, width = embed_weight.shape
    columns = points.shape[1] // LAT
    parts = width // LANES
    units, unit = send.shape
    vmem = pl.BlockSpec(memory_space=pltpu.VMEM)
    smem = pl.BlockSpec(memory_space=pltpu.SMEM)
    hbm = pl.BlockSpec(memory_space=pl.ANY)
    return pl.pallas_call(
        functools.partial(gather_kernel, columns, halo_turn),
        in_specs=[smem, smem, hbm, hbm, hbm, vmem, vmem],
        out_specs=hbm,
        out_shape=jax.ShapeDtypeStruct((units * unit, width), jnp.bfloat16),
        scratch_shapes=[
            pltpu.SMEM((units + 1,), jnp.int32),
            pltpu.SMEM((units * WINDOW + 1,), jnp.int32),
            pltpu.SMEM((units + 1,), jnp.int32),
            pltpu.SMEM((SLOTS,), jnp.int32),
            pltpu.SMEM((2, unit), jnp.int32),
            pltpu.VMEM((4, channels, LAT), jnp.bfloat16),
            pltpu.VMEM((SLOTS * LAT * parts, LANES), jnp.float32),
            pltpu.VMEM((CHUNK * parts, LANES), jnp.float32),
            pltpu.VMEM((CHUNK * parts, LANES), jnp.float32),
            pltpu.VMEM((2, CHUNK, width), jnp.bfloat16),
            pltpu.SemaphoreType.DMA((2,)),
            pltpu.SemaphoreType.DMA((4,)),
            pltpu.SemaphoreType.DMA((2,)),
        ],
        compiler_params=pltpu.CompilerParams(vmem_limit_bytes=40 << 20),
        cost_estimate=pl.CostEstimate(
            flops=2 * units * unit * channels * width,
            bytes_accessed=units * unit * width,
            transcendentals=units * unit * width // 2,
        ),
    )(low, high, send, points, points if halo is None else halo,
      embed_weight, embed_bias.reshape(1, -1))


def edge_kernel(
    columns,
    halo_turn,
    rows,
    low_ref,
    high_ref,
    gathered_ref,
    recv_ref,
    recv_row_ref,
    features_ref,
    start_ref,
    *refs,
):
    ways = lax.axis_size("ch")
    pieces = refs[:ways]
    (out_ref, list_ref, index, sender_all, receiver_all, recv_terms, feature_all, even, odd,
     held, hidden, index_sem, sem) = refs[ways:]
    me = lax.axis_index("ch")
    nodes, width = out_ref.shape
    part = width // ways
    parts = width // LANES
    unit = recv_ref.shape[1]
    rings = index.shape[0]
    count = pick_units(low_ref, high_ref, list_ref, columns, halo_turn)

    def fetch(n):
        slot = lax.rem(n, 2)
        start = pl.multiple_of(list_ref[n] * unit, unit)
        return pltpu.make_async_copy(
            gathered_ref.at[pl.ds(start, unit), :], held.at[slot], sem.at[slot]
        )

    def fetch_index(n):
        slot = lax.rem(n, rings)
        return pltpu.make_async_copy(
            recv_ref.at[list_ref[n]], index.at[slot], index_sem.at[slot]
        )

    @pl.when(count > 0)
    def _():
        fetch(0).start()
        fetch_index(0).start()

    pl.when(count > 1)(lambda: fetch_index(1).start())
    at = [sum(rows[:n]) for n in range(len(rows) + 1)]
    for j, piece in enumerate(pieces):
        lanes = slice(j * part, (j + 1) * part)
        sender_all[:, lanes] = piece[at[0]:at[1], :]
        receiver_all[:, lanes] = piece[at[1]:at[2], :]
        feature_all[:, lanes] = piece[at[3]:at[4], :]
    terms = jnp.zeros((nodes, width), jnp.float32)
    for j, piece in enumerate(pieces):
        owner = jnp.bitwise_xor(me, j)
        terms += jnp.dot(
            piece[at[2]:at[3], :],
            receiver_all[pl.ds(pl.multiple_of(owner * part, part), part), :],
            preferred_element_type=jnp.float32,
        )
    for j in range(parts):
        recv_terms[pl.ds(j, nodes, stride=parts), :] = terms[:, j * LANES:(j + 1) * LANES]
    if halo_turn:
        out_ref[...] = start_ref[...]
    else:
        out_ref[...] = jnp.zeros_like(out_ref)

    def gather(n, half, rows_held):
        slot = lax.rem(n, rings)
        for i in range(CHUNK):
            place = pl.multiple_of(index[slot, half * CHUNK + i], parts)
            rows_held[pl.ds(parts * i, parts), :] = recv_terms[pl.ds(place, parts), :]

    def activate(n, half, rows_held):
        start = pl.multiple_of(list_ref[n] * unit + half * CHUNK, CHUNK)
        mine = slice(half * CHUNK, (half + 1) * CHUNK)
        before = jnp.dot(
            held[lax.rem(n, 2), mine, :], sender_all[...], preferred_element_type=jnp.float32
        )
        before += lax.dot_general(
            features_ref[:, pl.ds(start, CHUNK)], feature_all[...], (((0,), (0,)), ((), ())),
            preferred_element_type=jnp.float32,
        )
        for j in range(parts):
            lanes = slice(j * LANES, (j + 1) * LANES)
            hidden[mine, lanes] = silu(
                before[:, lanes] + rows_held[pl.ds(j, CHUNK, stride=parts), :]
            ).astype(jnp.bfloat16)

    @pl.when(count > 0)
    def _():
        fetch_index(0).wait()
        gather(0, 0, even)

    def one_unit(n, carry):
        after = n + 1 < count
        pl.when(after)(lambda: fetch(n + 1).start())
        pl.when(n + 2 < count)(lambda: fetch_index(n + 2).start())
        pl.when(after)(lambda: fetch_index(n + 1).wait())
        fetch(n).wait()
        gather(n, 1, odd)
        activate(n, 0, even)
        gather(jnp.where(after, n + 1, n), 0, even)
        activate(n, 1, odd)
        ids = recv_row_ref[:, pl.ds(pl.multiple_of(list_ref[n] * unit, unit), unit)]
        by_node = jnp.where(
            lax.broadcasted_iota(jnp.int32, (nodes, unit), 0) == ids, 1.0, 0.0
        ).astype(jnp.bfloat16)
        out_ref[...] += jnp.dot(by_node, hidden[...], preferred_element_type=jnp.float32)
        return carry

    lax.fori_loop(0, count, one_unit, 0)


def node_sums(low, high, found, recv, recv_row, features, start, pieces, rows, columns, nodes,
              halo_turn):
    edges, width = found.shape
    units, unit = recv.shape
    parts = width // LANES
    vmem = pl.BlockSpec(memory_space=pltpu.VMEM)
    smem = pl.BlockSpec(memory_space=pltpu.SMEM)
    hbm = pl.BlockSpec(memory_space=pl.ANY)
    return pl.pallas_call(
        functools.partial(edge_kernel, columns, halo_turn, rows),
        in_specs=[smem, smem, hbm, hbm, vmem, vmem, vmem] + [vmem] * len(pieces),
        out_specs=vmem,
        out_shape=jax.ShapeDtypeStruct((nodes, width), jnp.float32),
        scratch_shapes=[
            pltpu.SMEM((units + 1,), jnp.int32),
            pltpu.SMEM((4, unit), jnp.int32),
            pltpu.VMEM((width, width), jnp.bfloat16),
            pltpu.VMEM((width, width), jnp.bfloat16),
            pltpu.VMEM((nodes * parts, LANES), jnp.float32),
            pltpu.VMEM((rows[3], width), jnp.bfloat16),
            pltpu.VMEM((CHUNK * parts, LANES), jnp.float32),
            pltpu.VMEM((CHUNK * parts, LANES), jnp.float32),
            pltpu.VMEM((2, unit, width), jnp.bfloat16),
            pltpu.VMEM((unit, width), jnp.bfloat16),
            pltpu.SemaphoreType.DMA((4,)),
            pltpu.SemaphoreType.DMA((2,)),
        ],
        compiler_params=pltpu.CompilerParams(vmem_limit_bytes=40 << 20),
        cost_estimate=pl.CostEstimate(
            flops=edges * width * (width + 2 * nodes) // 2,
            bytes_accessed=edges * width // 2,
            transcendentals=edges * width // 4,
        ),
    )(low, high, found, recv, recv_row, features, start, *pieces)


def across(me, bit):
    return me + bit - 2 * bit * lax.rem(me // bit, 2)


def swapped(block, bit, width):
    parts = block.shape[1] // width
    return jnp.concatenate(
        [block[:, (n ^ bit) * width:((n ^ bit) + 1) * width] for n in range(parts)], axis=1
    )


def tail_kernel(
    rows,
    totals_ref,
    recv_ref,
    message_bias_ref,
    *refs,
):
    ch_count = lax.axis_size("ch")
    messages, pieces = refs[:ch_count], refs[ch_count:2 * ch_count]
    (out_ref, near, onward, far, normed, give, near_send, near_recv, far_send, far_recv,
     back_send, back_recv) = refs[2 * ch_count:]
    me = lax.axis_index("ch")
    parts, part, width = normed.shape
    beside, opposite = across(me, 1), across(me, 2)
    partners = [beside, opposite, across(opposite, 1)]
    barrier = pltpu.get_barrier_semaphore()
    for partner in partners:
        pl.semaphore_signal(
            barrier, inc=1, device_id={"ch": partner}, device_id_type=pl.DeviceIdType.MESH
        )
    pl.semaphore_wait(barrier, ch_count - 1)

    def copy_to(source, target, send, recv, partner):
        return pltpu.make_async_remote_copy(
            src_ref=source, dst_ref=target, send_sem=send, recv_sem=recv,
            device_id={"ch": partner}, device_id_type=pl.DeviceIdType.MESH,
        )

    nears = [
        copy_to(totals_ref.at[block], near.at[n], near_send.at[n], near_recv.at[n], beside)
        for n, block in enumerate((partners[2], beside))
    ]
    for copy in nears:
        copy.start()
    nears[0].wait()
    onward[...] = (totals_ref[opposite] + swapped(near[0], 1, width)).astype(onward.dtype)
    pass_on = copy_to(onward, far, far_send.at[0], far_recv.at[0], opposite)
    pass_on.start()

    def tally(n, counts):
        nodes_here = lax.broadcasted_iota(jnp.int32, (part, LANES), 0) + me * part
        for i in range(8):
            ids = recv_ref[pl.ds(n * 8 + i, 1), :]
            counts = counts + jnp.where(nodes_here == ids, 1.0, 0.0)
        return counts

    counts = lax.fori_loop(
        0, recv_ref.shape[0] // 8, tally, jnp.zeros((part, LANES), jnp.float32)
    )
    aggregated = jnp.sum(counts, axis=1, keepdims=True) * message_bias_ref[...]
    nears[1].wait()
    sums = totals_ref[me] + swapped(near[1], 1, width)
    pass_on.wait()
    sums = sums + swapped(far[...].astype(jnp.float32), 2, width)
    for n in range(parts):
        rest = sums[:, n * width:(n + 1) * width]
        for _ in range(3):
            piece = rest.astype(jnp.bfloat16)
            aggregated += jnp.dot(
                piece, messages[n][...], preferred_element_type=jnp.float32
            )
            rest = rest - piece.astype(jnp.float32)
    centre = jnp.mean(aggregated, axis=1, keepdims=True)
    spread = jnp.mean(jnp.square(aggregated - centre), axis=1, keepdims=True)
    result = (aggregated - centre) * lax.rsqrt(spread + 1.0)
    for n in range(parts):
        normed[n] = result[:, n * width:(n + 1) * width]
    at = [sum(rows[:n]) for n in range(len(rows) + 1)]
    mine = pl.ds(pl.multiple_of(me * part, part), part)
    returns = []
    for j in (3, 2, 1, 0):
        owner = ([me] + partners)[j]
        small = pieces[j][at[3]:at[4], :].astype(jnp.float32)
        gain = small[7:8] + small[8:9] + small[9:10]
        shift = small[10:11] + small[11:12] + small[12:13]
        latent = pieces[j][pl.ds(at[2] + pl.multiple_of(me * part, part), part), :]
        block = (latent.astype(jnp.float32) + normed[owner] * gain + shift).astype(out_ref.dtype)
        if j == 0:
            out_ref[mine, :] = block
            continue
        give[j - 1] = block
        copy = copy_to(
            give.at[j - 1], out_ref.at[mine, :], back_send.at[j - 1], back_recv.at[j - 1], owner
        )
        copy.start()
        returns.append(copy)
    for copy in returns:
        copy.wait()


def finished(totals, recv, messages, message_bias, pieces, rows, nodes):
    ch_count = lax.axis_size("ch")
    part = nodes // ch_count
    full = totals.shape[1]
    width = full // ch_count
    vmem = pl.BlockSpec(memory_space=pltpu.VMEM)
    return pl.pallas_call(
        functools.partial(tail_kernel, rows),
        in_specs=[vmem] * (3 + 2 * ch_count),
        out_specs=vmem,
        out_shape=jax.ShapeDtypeStruct((nodes, width), jnp.bfloat16),
        scratch_shapes=[
            pltpu.VMEM((2, part, full), jnp.float32),
            pltpu.VMEM((part, full), jnp.bfloat16),
            pltpu.VMEM((part, full), jnp.bfloat16),
            pltpu.VMEM((ch_count, part, width), jnp.float32),
            pltpu.VMEM((ch_count - 1, part, width), jnp.bfloat16),
            pltpu.SemaphoreType.DMA((2,)),
            pltpu.SemaphoreType.DMA((2,)),
            pltpu.SemaphoreType.DMA((1,)),
            pltpu.SemaphoreType.DMA((1,)),
            pltpu.SemaphoreType.DMA((ch_count - 1,)),
            pltpu.SemaphoreType.DMA((ch_count - 1,)),
        ],
        compiler_params=pltpu.CompilerParams(
            vmem_limit_bytes=32 << 20, collective_id=1, has_side_effects=True
        ),
    )(totals.reshape(ch_count, part, full), recv, message_bias.reshape(1, -1), *messages, *pieces)


def on_device(
    grid_inputs,
    embed_weight,
    embed_bias,
    mesh_latent,
    edge_features,
    senders,
    receivers,
    sender_weight,
    receiver_weight,
    feature_weight,
    hidden_bias,
    message_weight,
    message_bias,
    norm_gain,
    norm_shift,
):
    lon_count, ch_count = lax.axis_size("lon"), lax.axis_size("ch")
    lon_place, ch_place = lax.axis_index("lon"), lax.axis_index("ch")
    assert ch_count == 4
    columns = grid_inputs.shape[0] // LAT
    assert columns >= WINDOW
    mesh_nodes = mesh_latent.shape[0]
    width = embed_weight.shape[1]
    parts = width // LANES
    edges = senders.shape[0]
    unit = UNIT
    assert edges % unit == 0 and unit == 2 * CHUNK
    points = grid_inputs.T

    edge_start = jnp.where(ch_place == 0, (columns - HALO) * LAT, 0)
    edge_columns = lax.dynamic_slice(points, (0, edge_start), (points.shape[0], HALO * LAT))
    hops = []
    for i in range(lon_count):
        hops.append((i * ch_count, (i + 1) % lon_count * ch_count))
        hops.append(
            (i * ch_count + ch_count - 1, (i - 1) % lon_count * ch_count + ch_count - 1)
        )
    with jax.named_scope("halo_hop"):
        halo = lax.ppermute(edge_columns, ("lon", "ch"), hops)

    cut = lambda v: lax.reduce_precision(v, exponent_bits=8, mantissa_bits=7)

    def thirds(v):
        high = cut(v)
        mid = cut(v - high)
        return [high, mid, v - high - mid]

    components = edge_features.shape[0]
    singles = thirds(hidden_bias) + thirds(norm_gain) + thirds(norm_shift)
    pad = 16 - components - len(singles)
    small = jnp.concatenate(
        [
            feature_weight,
            jnp.stack(singles).astype(jnp.bfloat16),
            jnp.zeros((pad, feature_weight.shape[1]), jnp.bfloat16),
        ]
    )
    blocks = (sender_weight, receiver_weight, mesh_latent, small)
    rows = tuple(block.shape[0] for block in blocks)
    swap = lambda v: [v] + [
        lax.ppermute(v, "ch", [(i, i ^ j) for i in range(ch_count)]) for j in range(1, ch_count)
    ]
    with jax.named_scope("weights_hop"):
        pieces = swap(jnp.concatenate(blocks))
    with jax.named_scope("messages_hop"):
        messages = swap(message_weight)

    shifted = jnp.mod(senders // LAT - lon_place * columns + HALO, columns * lon_count)
    by_unit = shifted.reshape(-1, unit)
    low, high = jnp.min(by_unit, axis=1), jnp.max(by_unit, axis=1)
    send = ((shifted % SLOTS * LAT + senders % LAT) * parts).reshape(-1, unit)
    recv = receivers - lon_place * mesh_nodes
    features = jnp.concatenate(
        [
            edge_features,
            jnp.ones((3, edges), jnp.bfloat16),
            jnp.zeros((16 - components - 3, edges), jnp.bfloat16),
        ]
    )

    totals = jnp.zeros((8, LANES), jnp.float32)
    for halo_turn in (False, True):
        with jax.named_scope("halo_work" if halo_turn else "inner_work"):
            found = gathered(
                low, high, send, points, halo if halo_turn else None, embed_weight, embed_bias,
                halo_turn,
            )
            totals = node_sums(
                low, high, found, (recv * parts).reshape(-1, unit), recv.reshape(1, -1),
                features, totals, pieces, rows, columns, mesh_nodes, halo_turn,
            )
    return finished(
        totals, recv.reshape(-1, LANES), messages, message_bias, pieces, rows, mesh_nodes
    )


def solution(mesh):
    return jax.shard_map(
        on_device,
        mesh=mesh,
        in_specs=(
            P("lon", None),
            P(),
            P(),
            P("lon", "ch"),
            P(None, "lon"),
            P("lon"),
            P("lon"),
            P(None, "ch"),
            P(None, "ch"),
            P(None, "ch"),
            P("ch"),
            P("ch", None),
            P(),
            P("ch"),
            P("ch"),
        ),
        out_specs=P("lon", "ch"),
        check_vma=False,
    )
```

```python
import functools

import jax
import jax.numpy as jnp
from jax import lax
from jax.experimental import pallas as pl
from jax.experimental.pallas import tpu as pltpu
from jax.sharding import PartitionSpec as P


LAT = 640
HALO = 4
UNIT = 512
WINDOW = 7
SLOTS = 8
PARTS = 4
LANES = 128
CHUNK = 256


def silu_of_double(half):
    return half + half * jnp.tanh(half)


def low_of(bounds_ref, u):
    return bounds_ref[0, u * (UNIT // LANES)]


def high_of(bounds_ref, u):
    return bounds_ref[1, u * (UNIT // LANES)]


def pick_units(bounds_ref, list_ref, units, columns, halo_turn):
    me = lax.axis_index("ch")
    ch_count = lax.axis_size("ch")
    one = lambda flag: jnp.where(flag, 1, 0)
    at_left = [one(low_of(bounds_ref, u) < HALO) for u in range(units)]
    at_right = [one(high_of(bounds_ref, u) >= HALO + columns) for u in range(units)]
    lefts, rights = sum(at_left), sum(at_right)
    inner_count = units - lefts - rights
    end_share = -(-units // ch_count)
    first = jnp.minimum(jnp.maximum(end_share - lefts, 0), inner_count)
    last = jnp.maximum(inner_count - jnp.maximum(end_share - rights, 0), first)
    middle = lambda k: first + lax.div((last - first) * (k - 1), ch_count - 2)
    begin = jnp.where(me == 0, 0, middle(me))
    end = jnp.where(me == ch_count - 1, inner_count, middle(me + 1))
    first_turn = -(-units * 5 // (8 * ch_count))
    count, rank = jnp.int32(0), jnp.int32(0)
    for u in range(units):
        inner = 1 - at_left[u] - at_right[u]
        if halo_turn:
            inside = jnp.logical_and(rank >= begin + first_turn, rank < end)
            at_mine = jnp.where(me == 0, at_left[u], 0) + jnp.where(
                me == ch_count - 1, at_right[u], 0
            )
            mine = jnp.where(inside, inner, at_mine)
        else:
            inside = jnp.logical_and(
                rank >= begin, rank < jnp.minimum(begin + first_turn, end)
            )
            mine = jnp.where(inside, inner, 0)
        list_ref[count] = u
        count = count + mine
        rank = rank + inner
    return count


def spread(ref, ids):
    for n in range(ids.shape[0] // 8):
        tile = ids[8 * n:8 * n + 8]
        ref[16 * n:16 * n + 8, :] = tile
        ref[16 * n + 8:16 * n + 16, :] = pltpu.roll(tile, 4, 0)


def prepare_kernel(
    columns,
    x_ref,
    *refs,
):
    sources, refs = refs[:10], refs[10:]
    (edge_ref, packed_ref, send_ref, recv_ref, place_ref, bounds_ref, buffer, packed,
     senders_ref, receivers_ref, feature_ref, bias_ref, gain_ref, shift_ref,
     in_sem, out_sem, pack_sem, source_sem) = refs
    lon_count = lax.axis_size("lon")
    lon_place, ch_place = lax.axis_index("lon"), lax.axis_index("ch")
    start = jnp.where(ch_place == 0, (columns - HALO) * LAT, 0)
    takes = [
        pltpu.make_async_copy(
            x_ref.at[:, pl.ds(pl.multiple_of(start + n * LAT, LANES), LAT)],
            buffer.at[n],
            in_sem.at[n],
        )
        for n in range(HALO)
    ]
    gives = [
        pltpu.make_async_copy(
            buffer.at[n], edge_ref.at[:, pl.ds(n * LAT, LAT)], out_sem.at[n]
        )
        for n in range(HALO)
    ]
    targets = [senders_ref, receivers_ref]
    row = 0
    for ref in sources[2:5]:
        targets.append(packed.at[pl.ds(row, ref.shape[0]), :])
        row += ref.shape[0]
    targets += [feature_ref, bias_ref, gain_ref, shift_ref]
    loads = [
        pltpu.make_async_copy(source, target, source_sem.at[n])
        for n, (source, target) in enumerate(zip(sources, targets))
    ]
    tall, part = sources[9].shape[0], packed.shape[1]
    loads += [
        pltpu.make_async_copy(
            sources[9].at[:, pl.ds(n * part, part)],
            packed.at[pl.ds(row + 16 + n * tall, tall), :],
            source_sem.at[9 + n],
        )
        for n in range(sources[9].shape[1] // part)
    ]
    for copy in takes + loads:
        copy.start()
    for copy in loads:
        copy.wait()
    singles = [feature_ref[...].astype(jnp.float32)]
    for ref in (bias_ref, gain_ref, shift_ref):
        rest = ref[...]
        for _ in range(3):
            high = rest.astype(jnp.bfloat16).astype(jnp.float32)
            singles.append(high)
            rest = rest - high
    used = feature_ref.shape[0] + len(singles) - 1
    singles.append(jnp.zeros((16 - used, singles[0].shape[1]), jnp.float32))
    packed[row:row + 16, :] = jnp.concatenate(singles).astype(jnp.bfloat16)
    pack = pltpu.make_async_copy(packed, packed_ref, pack_sem)
    pack.start()

    senders = senders_ref[...]
    column = lax.shift_right_logical(
        lax.shift_right_logical(senders, 7) * 52429, 18
    )
    latitude = senders - column * LAT
    total = columns * lon_count
    column = column - lon_place * columns + HALO
    column = jnp.where(column < 0, column + total, column)
    column = jnp.where(column >= total, column - total, column)
    parts = PARTS
    spread(send_ref, (jnp.bitwise_and(column, SLOTS - 1) * LAT + latitude) * parts)
    recv = receivers_ref[...] - lon_place * sources[4].shape[0]
    recv_ref[...] = recv
    spread(place_ref, recv * parts)
    tall = -(-senders.shape[0] // LANES) * LANES
    for n, (pick, near, fill) in enumerate(
        ((jnp.min, jnp.minimum, total), (jnp.max, jnp.maximum, 0))
    ):
        best = column
        for shift in (1, 2):
            best = near(best, pltpu.roll(best, best.shape[0] - shift, 0))
        best = jnp.concatenate(
            [best, jnp.full((tall - best.shape[0], LANES), fill, jnp.int32)]
        )
        bounds_ref[n:n + 1, :] = pick(jnp.transpose(best), axis=0, keepdims=True)
    for take, give in zip(takes, gives):
        take.wait()
        give.start()
    for give in gives:
        give.wait()
    pack.wait()


def prepared(points, senders, receivers, sender_weight, receiver_weight, mesh_latent,
             feature_weight, hidden_bias, norm_gain, norm_shift, message_weight):
    columns = points.shape[1] // LAT
    assert LAT == 5 * LANES and lax.axis_size("lon") * points.shape[1] // LANES < 40960
    rows = senders.shape[0] // LANES
    part = sender_weight.shape[1]
    packed_rows = (
        2 * sender_weight.shape[0] + receiver_weight.shape[0] + mesh_latent.shape[0] + 16
    )
    vmem = pl.BlockSpec(memory_space=pltpu.VMEM)
    hbm = pl.BlockSpec(memory_space=pltpu.HBM)
    ids = jax.ShapeDtypeStruct((rows, LANES), jnp.int32)
    wide_ids = jax.ShapeDtypeStruct((2 * rows, LANES), jnp.int32)
    assert rows % 8 == 0 and UNIT == 4 * LANES
    return pl.pallas_call(
        functools.partial(prepare_kernel, columns),
        in_specs=[hbm] * 11,
        out_specs=[hbm, hbm, vmem, vmem, vmem, vmem],
        out_shape=[
            jax.ShapeDtypeStruct((points.shape[0], HALO * LAT), points.dtype),
            jax.ShapeDtypeStruct((packed_rows, part), jnp.bfloat16),
            wide_ids,
            ids,
            wide_ids,
            jax.ShapeDtypeStruct((2, -(-rows // LANES) * LANES), jnp.int32),
        ],
        scratch_shapes=[
            pltpu.VMEM((HALO, points.shape[0], LAT), points.dtype),
            pltpu.VMEM((packed_rows, part), jnp.bfloat16),
            pltpu.VMEM((rows, LANES), jnp.int32),
            pltpu.VMEM((rows, LANES), jnp.int32),
            pltpu.VMEM(feature_weight.shape, jnp.bfloat16),
            pltpu.VMEM((1, part), jnp.float32),
            pltpu.VMEM((1, part), jnp.float32),
            pltpu.VMEM((1, part), jnp.float32),
            pltpu.SemaphoreType.DMA((HALO,)),
            pltpu.SemaphoreType.DMA((HALO,)),
            pltpu.SemaphoreType.DMA,
            pltpu.SemaphoreType.DMA((9 + PARTS,)),
        ],
        compiler_params=pltpu.CompilerParams(vmem_limit_bytes=63 << 20),
    )(points, senders.reshape(rows, LANES), receivers.reshape(rows, LANES), sender_weight,
      receiver_weight, mesh_latent, feature_weight, hidden_bias.reshape(1, -1),
      norm_gain.reshape(1, -1), norm_shift.reshape(1, -1), message_weight)


def index_rows(u):
    return pl.ds(pl.multiple_of(u * 8, 8), 8)


def gather_kernel(
    columns,
    halo_turn,
    bounds_ref,
    send_ref,
    x_ref,
    halo_ref,
    embed_ref,
    bias_ref,
    out_ref,
    list_ref,
    events,
    event_at,
    held_column,
    index_even,
    index_odd,
    points,
    table,
    even,
    odd,
    packed,
    embed_half,
    index_sem,
    point_sem,
    out_sem,
):
    index = (index_even, index_odd)
    parts = out_ref.shape[1] // LANES
    unit = UNIT
    step = LAT * parts
    depth = points.shape[0]
    count = pick_units(bounds_ref, list_ref, list_ref.shape[0] - 1, columns, halo_turn)

    embed_half[...] = embed_ref[...] * jnp.bfloat16(0.5)
    for n in range(SLOTS):
        held_column[n] = -1

    def note_unit(n, total):
        u = list_ref[n]
        event_at[n] = total

        def note(column, total):
            slot = lax.rem(column, SLOTS)
            new = jnp.where(held_column[slot] == column, 0, 1)
            held_column[slot] = column
            events[total] = column
            return total + new

        return lax.fori_loop(
            low_of(bounds_ref, u), high_of(bounds_ref, u) + 1, note, total
        )

    total = lax.fori_loop(0, count, note_unit, jnp.int32(0))
    event_at[count] = total

    def fetch(event):
        column, slot = events[event], lax.rem(event, depth)

        def copy(source, place):
            start = pl.multiple_of(place * LAT, LANES)
            return pltpu.make_async_copy(
                source.at[:, pl.ds(start, LAT)], points.at[slot], point_sem.at[slot]
            )

        if not halo_turn:
            copy(x_ref, column - HALO).start()
            return
        last = column >= HALO + columns
        outside = jnp.logical_or(column < HALO, last)
        pl.when(outside)(
            lambda: copy(halo_ref, jnp.where(last, column - HALO - columns, column)).start()
        )
        pl.when(jnp.logical_not(outside))(lambda: copy(x_ref, column - HALO).start())

    def fetch_index(n, slot):
        return pltpu.make_async_copy(
            send_ref.at[index_rows(list_ref[n]), :], index[slot], index_sem.at[slot]
        )

    for event in range(depth):
        pl.when(event < total)(functools.partial(fetch, event))
    for n in range(2):
        pl.when(n < count)(lambda n=n: fetch_index(n, n).start())

    def one_event(event, carry):
        slot = lax.rem(event, depth)
        pltpu.make_async_copy(
            x_ref.at[:, pl.ds(0, LAT)], points.at[slot], point_sem.at[slot]
        ).wait()
        before = lax.dot_general(
            points[slot], embed_half[...], (((0,), (0,)), ((), ())),
            preferred_element_type=jnp.float32,
        ) + 0.5 * bias_ref[...]
        latent = silu_of_double(before)
        base = lax.rem(events[event], SLOTS) * step
        for j in range(parts):
            table[pl.ds(base + j, LAT, stride=parts), :] = latent[:, j * LANES:(j + 1) * LANES]
        pl.when(event + depth < total)(lambda: fetch(event + depth))
        return carry

    def gather(slot, half, held):
        row = half * (CHUNK // LANES)
        for i in range(CHUNK):
            place = pl.multiple_of(index[slot][row + i // LANES, i % LANES], parts)
            held[pl.ds(parts * i, parts), :] = table[pl.ds(place, parts), :]

    def leave(start, slot, held):
        for j in range(parts):
            packed[slot, :, j * LANES:(j + 1) * LANES] = (
                held[pl.ds(j, CHUNK, stride=parts), :].astype(jnp.bfloat16)
            )
        pltpu.make_async_copy(
            packed.at[slot],
            out_ref.at[pl.ds(pl.multiple_of(start, CHUNK), CHUNK), :],
            out_sem.at[slot],
        ).start()

    def settle(slot):
        pltpu.make_async_copy(
            packed.at[slot], out_ref.at[pl.ds(0, CHUNK), :], out_sem.at[slot]
        ).wait()

    spare = out_ref.shape[0] - CHUNK

    def second_half(n):
        earlier = list_ref[jnp.maximum(n - 1, 0)] * unit + CHUNK
        return jnp.where(n > 0, earlier, spare)

    def one_unit(n, turn):
        lax.fori_loop(event_at[n], event_at[n + 1], one_event, 0)
        fetch_index(n, turn).wait()
        for slot in (turn, 2 + turn):
            pl.when(n > 1)(functools.partial(settle, slot))
        leave(second_half(n), 2 + turn, odd)
        gather(turn, 0, even)
        leave(list_ref[n] * unit, turn, even)
        gather(turn, 1, odd)
        pl.when(n + 2 < count)(lambda: fetch_index(n + 2, turn).start())

    def two_units(m, carry):
        one_unit(2 * m, 0)
        pl.when(2 * m + 1 < count)(lambda: one_unit(2 * m + 1, 1))
        return carry

    lax.fori_loop(0, (count + 1) // 2, two_units, 0)

    @pl.when(count > 0)
    def _():
        turn = lax.rem(count, 2)
        for slot in (turn, 2 + turn):
            pl.when(count > 1)(functools.partial(settle, slot))
        leave(second_half(count), 2 + turn, odd)
        settle(2 + turn)
        for slot in (1 - turn, 3 - turn):
            settle(slot)


def gathered(bounds, send, points, halo, embed_weight, embed_bias, halo_turn):
    channels, width = embed_weight.shape
    columns = points.shape[1] // LAT
    parts = width // LANES
    unit = UNIT
    units = send.shape[0] // 8
    vmem = pl.BlockSpec(memory_space=pltpu.VMEM)
    smem = pl.BlockSpec(memory_space=pltpu.SMEM)
    hbm = pl.BlockSpec(memory_space=pltpu.HBM)
    return pl.pallas_call(
        functools.partial(gather_kernel, columns, halo_turn),
        in_specs=[smem, hbm, hbm, hbm, vmem, vmem],
        out_specs=hbm,
        out_shape=jax.ShapeDtypeStruct((units * unit + CHUNK, width), jnp.bfloat16),
        scratch_shapes=[
            pltpu.SMEM((units + 1,), jnp.int32),
            pltpu.SMEM((units * WINDOW + 1,), jnp.int32),
            pltpu.SMEM((units + 1,), jnp.int32),
            pltpu.SMEM((SLOTS,), jnp.int32),
            pltpu.SMEM((8, LANES), jnp.int32),
            pltpu.SMEM((8, LANES), jnp.int32),
            pltpu.VMEM((6, channels, LAT), jnp.bfloat16),
            pltpu.VMEM((SLOTS * LAT * parts, LANES), jnp.float32),
            pltpu.VMEM((CHUNK * parts, LANES), jnp.float32),
            pltpu.VMEM((CHUNK * parts, LANES), jnp.float32),
            pltpu.VMEM((4, CHUNK, width), jnp.bfloat16),
            pltpu.VMEM((channels, width), jnp.bfloat16),
            pltpu.SemaphoreType.DMA((2,)),
            pltpu.SemaphoreType.DMA((6,)),
            pltpu.SemaphoreType.DMA((4,)),
        ],
        compiler_params=pltpu.CompilerParams(vmem_limit_bytes=40 << 20),
        cost_estimate=pl.CostEstimate(
            flops=2 * units * unit * channels * width,
            bytes_accessed=units * unit * width,
            transcendentals=units * unit * width // 2,
        ),
    )(bounds, send, points, points if halo is None else halo,
      embed_weight, embed_bias.reshape(1, -1))


def edge_kernel(
    columns,
    halo_turn,
    rows,
    bounds_ref,
    gathered_ref,
    place_ref,
    recv_ref,
    features_ref,
    start_ref,
    *refs,
):
    ways = lax.axis_size("ch")
    pieces = refs[:ways]
    (out_ref, list_ref, index, sender_all, receiver_all, recv_terms, feature_all, even, odd,
     held, hidden, index_sem, sem) = refs[ways:]
    me = lax.axis_index("ch")
    nodes, width = out_ref.shape
    part = width // ways
    parts = width // LANES
    unit = UNIT
    rings = index.shape[0]
    count = pick_units(bounds_ref, list_ref, list_ref.shape[0] - 1, columns, halo_turn)

    def fetch(n):
        slot = lax.rem(n, rings)
        start = pl.multiple_of(list_ref[n] * unit, unit)
        return pltpu.make_async_copy(
            gathered_ref.at[pl.ds(start, unit), :], held.at[slot], sem.at[slot]
        )

    def fetch_index(n):
        slot = lax.rem(n, rings)
        return pltpu.make_async_copy(
            place_ref.at[index_rows(list_ref[n]), :], index.at[slot], index_sem.at[slot]
        )

    def fetch_both(n):
        fetch_index(n).start()
        fetch(n).start()

    for n in range(rings - 2):
        pl.when(n < count)(functools.partial(fetch_both, n))
    at = [sum(rows[:n]) for n in range(len(rows) + 1)]
    for j, piece in enumerate(pieces):
        lanes = slice(j * part, (j + 1) * part)
        sender_all[:, lanes] = piece[at[0]:at[1], :] * jnp.bfloat16(0.5)
        receiver_all[:, lanes] = piece[at[1]:at[2], :]
        feature_all[:, lanes] = piece[at[3]:at[4], :] * jnp.bfloat16(0.5)
    components = features_ref.shape[0]
    singles = jnp.concatenate([piece[at[3]:at[4], :] for piece in pieces], axis=1)
    singles = singles.astype(jnp.float32)
    terms = jnp.broadcast_to(
        singles[components:components + 1] + singles[components + 1:components + 2]
        + singles[components + 2:components + 3],
        (nodes, width),
    )
    for j, piece in enumerate(pieces):
        owner = jnp.bitwise_xor(me, j)
        terms += jnp.dot(
            piece[at[2]:at[3], :],
            receiver_all[pl.ds(pl.multiple_of(owner * part, part), part), :],
            preferred_element_type=jnp.float32,
        )
    for j in range(parts):
        recv_terms[pl.ds(j, nodes, stride=parts), :] = (
            0.5 * terms[:, j * LANES:(j + 1) * LANES]
        )
    if halo_turn:
        out_ref[...] = start_ref[...]
    else:
        out_ref[...] = jnp.zeros_like(out_ref)

    def gather(n, rows_held):
        slot = lax.rem(n, rings)
        for i in range(unit):
            place = pl.multiple_of(index[slot, i // LANES, i % LANES], parts)
            rows_held[pl.ds(parts * i, parts), :] = recv_terms[pl.ds(place, parts), :]

    def activate(n, turn, rows_held):
        start = pl.multiple_of(list_ref[n] * unit, unit)
        mine = slice(turn * unit, (turn + 1) * unit)
        before = jnp.dot(
            held[lax.rem(n, rings)], sender_all[...], preferred_element_type=jnp.float32
        )
        before += lax.dot_general(
            features_ref[:, pl.ds(start, unit)], feature_all[:components, :],
            (((0,), (0,)), ((), ())),
            preferred_element_type=jnp.float32,
        )
        for j in range(parts):
            lanes = slice(j * LANES, (j + 1) * LANES)
            hidden[mine, lanes] = silu_of_double(
                before[:, lanes] + rows_held[pl.ds(j, unit, stride=parts), :]
            ).astype(jnp.bfloat16)

    def add_up(first, number):
        each = lax.broadcasted_iota(jnp.int32, (nodes, LANES), 0)
        by_node = jnp.concatenate(
            [
                jnp.where(
                    each == recv_ref[pl.ds(list_ref[first + n] * (unit // LANES) + b, 1), :],
                    1.0,
                    0.0,
                )
                for n in range(number)
                for b in range(unit // LANES)
            ],
            axis=1,
        ).astype(jnp.bfloat16)
        out_ref[...] += jnp.dot(
            by_node, hidden[:number * unit, :], preferred_element_type=jnp.float32
        )

    @pl.when(count > 0)
    def _():
        fetch_index(0).wait()
        gather(0, even)

    def pair(m, carry):
        first, second = 2 * m, 2 * m + 1
        after = second + 1 < count
        for n in (first, second):
            pl.when(n + rings - 2 < count)(functools.partial(fetch_both, n + rings - 2))
        fetch_index(second).wait()
        fetch(first).wait()
        gather(second, odd)
        activate(first, 0, even)
        pl.when(after)(lambda: fetch_index(second + 1).wait())
        fetch(second).wait()
        gather(jnp.where(after, second + 1, second), even)
        activate(second, 1, odd)
        add_up(first, 2)
        return carry

    lax.fori_loop(0, count // 2, pair, 0)

    @pl.when(lax.rem(count, 2) == 1)
    def _():
        fetch(count - 1).wait()
        activate(count - 1, 0, even)
        add_up(count - 1, 1)


def node_sums(bounds, found, place, recv, features, start, pieces, rows, columns, nodes,
              halo_turn):
    edges, width = found.shape
    unit = UNIT
    units = place.shape[0] // 8
    parts = width // LANES
    vmem = pl.BlockSpec(memory_space=pltpu.VMEM)
    smem = pl.BlockSpec(memory_space=pltpu.SMEM)
    hbm = pl.BlockSpec(memory_space=pltpu.HBM)
    return pl.pallas_call(
        functools.partial(edge_kernel, columns, halo_turn, rows),
        in_specs=[smem, hbm, hbm, vmem, vmem, vmem] + [vmem] * len(pieces),
        out_specs=vmem,
        out_shape=jax.ShapeDtypeStruct((nodes, width), jnp.float32),
        scratch_shapes=[
            pltpu.SMEM((units + 1,), jnp.int32),
            pltpu.SMEM((6, 8, LANES), jnp.int32),
            pltpu.VMEM((width, width), jnp.bfloat16),
            pltpu.VMEM((width, width), jnp.bfloat16),
            pltpu.VMEM((nodes * parts, LANES), jnp.float32),
            pltpu.VMEM((rows[3], width), jnp.bfloat16),
            pltpu.VMEM((unit * parts, LANES), jnp.float32),
            pltpu.VMEM((unit * parts, LANES), jnp.float32),
            pltpu.VMEM((6, unit, width), jnp.bfloat16),
            pltpu.VMEM((2 * unit, width), jnp.bfloat16),
            pltpu.SemaphoreType.DMA((6,)),
            pltpu.SemaphoreType.DMA((6,)),
        ],
        compiler_params=pltpu.CompilerParams(vmem_limit_bytes=40 << 20),
        cost_estimate=pl.CostEstimate(
            flops=edges * width * (width + 2 * nodes) // 2,
            bytes_accessed=edges * width // 2,
            transcendentals=edges * width // 4,
        ),
    )(bounds, found, place, recv, features, start, *pieces)


def swap_kernel(own_ref, far_ref, own_out, far_out, send, recv):
    beside = across(lax.axis_index("ch"), 1)
    barrier = pltpu.get_barrier_semaphore()
    pl.semaphore_signal(
        barrier, inc=1, device_id={"ch": beside}, device_id_type=pl.DeviceIdType.MESH
    )
    pl.semaphore_wait(barrier, 1)
    copies = [
        pltpu.make_async_remote_copy(
            src_ref=source, dst_ref=target, send_sem=send.at[n], recv_sem=recv.at[n],
            device_id={"ch": beside}, device_id_type=pl.DeviceIdType.MESH,
        )
        for n, (source, target) in enumerate(((own_ref, own_out), (far_ref, far_out)))
    ]
    for copy in copies:
        copy.start()
    for copy in copies:
        copy.wait()


def swapped_beside(own, far):
    vmem = pl.BlockSpec(memory_space=pltpu.VMEM)
    return pl.pallas_call(
        swap_kernel,
        in_specs=[vmem] * 2,
        out_specs=[vmem] * 2,
        out_shape=[jax.ShapeDtypeStruct(own.shape, own.dtype)] * 2,
        scratch_shapes=[pltpu.SemaphoreType.DMA((2,)), pltpu.SemaphoreType.DMA((2,))],
        compiler_params=pltpu.CompilerParams(
            vmem_limit_bytes=8 << 20, collective_id=0, has_side_effects=True
        ),
    )(own, far)


def across(me, bit):
    return me + bit - 2 * bit * lax.rem(me // bit, 2)


def swapped(block, bit, width):
    parts = block.shape[1] // width
    return jnp.concatenate(
        [block[:, (n ^ bit) * width:((n ^ bit) + 1) * width] for n in range(parts)], axis=1
    )


def tail_kernel(
    rows,
    totals_ref,
    recv_ref,
    message_bias_ref,
    *refs,
):
    ch_count = lax.axis_size("ch")
    pieces = refs[:ch_count]
    (out_ref, near, onward, far, normed, give, near_send, near_recv, far_send, far_recv,
     back_send, back_recv, messages) = refs[ch_count:]
    me = lax.axis_index("ch")
    parts, part, width = normed.shape
    beside, opposite = across(me, 1), across(me, 2)
    partners = [beside, opposite, across(opposite, 1)]
    barrier = pltpu.get_barrier_semaphore()
    for partner in partners:
        pl.semaphore_signal(
            barrier, inc=1, device_id={"ch": partner}, device_id_type=pl.DeviceIdType.MESH
        )
    pl.semaphore_wait(barrier, ch_count - 1)

    def copy_to(source, target, send, recv, partner):
        return pltpu.make_async_remote_copy(
            src_ref=source, dst_ref=target, send_sem=send, recv_sem=recv,
            device_id={"ch": partner}, device_id_type=pl.DeviceIdType.MESH,
        )

    nears = [
        copy_to(totals_ref.at[block], near.at[n], near_send.at[n], near_recv.at[n], beside)
        for n, block in enumerate((partners[2], beside))
    ]
    for copy in nears:
        copy.start()
    at = [sum(rows[:n]) for n in range(len(rows) + 1)]
    for n in range(parts):
        for j in range(parts):
            first = at[4] + j * width
            messages[n, :, j * width:(j + 1) * width] = pieces[n][first:first + width, :]
    nears[0].wait()
    onward[...] = (totals_ref[opposite] + swapped(near[0], 1, width)).astype(onward.dtype)
    pass_on = copy_to(onward, far, far_send.at[0], far_recv.at[0], opposite)
    pass_on.start()

    def tally(n, counts):
        nodes_here = lax.broadcasted_iota(jnp.int32, (part, LANES), 0) + me * part
        for i in range(8):
            ids = recv_ref[pl.ds(n * 8 + i, 1), :]
            counts = counts + jnp.where(nodes_here == ids, 1.0, 0.0)
        return counts

    counts = lax.fori_loop(
        0, recv_ref.shape[0] // 8, tally, jnp.zeros((part, LANES), jnp.float32)
    )
    aggregated = jnp.sum(counts, axis=1, keepdims=True) * message_bias_ref[...]
    nears[1].wait()
    sums = totals_ref[me] + swapped(near[1], 1, width)
    pass_on.wait()
    sums = sums + swapped(far[...].astype(jnp.float32), 2, width)
    for n in range(parts):
        rest = sums[:, n * width:(n + 1) * width]
        for _ in range(2):
            piece = rest.astype(jnp.bfloat16)
            aggregated += jnp.dot(
                piece, messages[n], preferred_element_type=jnp.float32
            )
            rest = rest - piece.astype(jnp.float32)
    centre = jnp.mean(aggregated, axis=1, keepdims=True)
    spread = jnp.mean(jnp.square(aggregated - centre), axis=1, keepdims=True)
    result = (aggregated - centre) * lax.rsqrt(spread + 1.0)
    for n in range(parts):
        normed[n] = result[:, n * width:(n + 1) * width]
    mine = pl.ds(pl.multiple_of(me * part, part), part)
    returns = []
    for j in (3, 2, 1, 0):
        owner = ([me] + partners)[j]
        small = pieces[j][at[3]:at[4], :].astype(jnp.float32)
        gain = small[7:8] + small[8:9] + small[9:10]
        shift = small[10:11] + small[11:12] + small[12:13]
        latent = pieces[j][pl.ds(at[2] + pl.multiple_of(me * part, part), part), :]
        block = (latent.astype(jnp.float32) + normed[owner] * gain + shift).astype(out_ref.dtype)
        if j == 0:
            out_ref[mine, :] = block
            continue
        give[j - 1] = block
        copy = copy_to(
            give.at[j - 1], out_ref.at[mine, :], back_send.at[j - 1], back_recv.at[j - 1], owner
        )
        copy.start()
        returns.append(copy)
    for copy in returns:
        copy.wait()


def finished(totals, recv, message_bias, pieces, rows, nodes):
    ch_count = lax.axis_size("ch")
    part = nodes // ch_count
    full = totals.shape[1]
    width = full // ch_count
    vmem = pl.BlockSpec(memory_space=pltpu.VMEM)
    return pl.pallas_call(
        functools.partial(tail_kernel, rows),
        in_specs=[vmem] * (3 + ch_count),
        out_specs=vmem,
        out_shape=jax.ShapeDtypeStruct((nodes, width), jnp.bfloat16),
        scratch_shapes=[
            pltpu.VMEM((2, part, full), jnp.float32),
            pltpu.VMEM((part, full), jnp.bfloat16),
            pltpu.VMEM((part, full), jnp.bfloat16),
            pltpu.VMEM((ch_count, part, width), jnp.float32),
            pltpu.VMEM((ch_count - 1, part, width), jnp.bfloat16),
            pltpu.SemaphoreType.DMA((2,)),
            pltpu.SemaphoreType.DMA((2,)),
            pltpu.SemaphoreType.DMA((1,)),
            pltpu.SemaphoreType.DMA((1,)),
            pltpu.SemaphoreType.DMA((ch_count - 1,)),
            pltpu.SemaphoreType.DMA((ch_count - 1,)),
            pltpu.VMEM((ch_count, width, full), jnp.bfloat16),
        ],
        compiler_params=pltpu.CompilerParams(
            vmem_limit_bytes=32 << 20, collective_id=1, has_side_effects=True
        ),
    )(totals.reshape(ch_count, part, full), recv, message_bias.reshape(1, -1), *pieces)


def on_device(
    grid_inputs,
    embed_weight,
    embed_bias,
    mesh_latent,
    edge_features,
    senders,
    receivers,
    sender_weight,
    receiver_weight,
    feature_weight,
    hidden_bias,
    message_weight,
    message_bias,
    norm_gain,
    norm_shift,
):
    lon_count, ch_count = lax.axis_size("lon"), lax.axis_size("ch")
    assert ch_count == 4
    columns = grid_inputs.shape[0] // LAT
    assert columns >= WINDOW
    mesh_nodes = mesh_latent.shape[0]
    width = embed_weight.shape[1]
    assert width == PARTS * LANES
    edges = senders.shape[0]
    unit = UNIT
    assert edges % unit == 0 and unit == 2 * CHUNK
    points = grid_inputs.T

    edge_columns, packed, send, recv, place, bounds = prepared(
        points, senders, receivers, sender_weight, receiver_weight, mesh_latent,
        feature_weight, hidden_bias, norm_gain, norm_shift, message_weight,
    )
    rows = (width, width, mesh_nodes, 16)
    hops = []
    for i in range(lon_count):
        hops.append((i * ch_count, (i + 1) % lon_count * ch_count))
        hops.append(
            (i * ch_count + ch_count - 1, (i - 1) % lon_count * ch_count + ch_count - 1)
        )
    halo = lax.ppermute(edge_columns, ("lon", "ch"), hops)

    opposite = lax.ppermute(packed, "ch", [(i, i ^ 2) for i in range(ch_count)])
    beside, diagonal = swapped_beside(packed, opposite)
    pieces = [packed, beside, opposite, diagonal]

    totals = jnp.zeros((8, LANES), jnp.float32)
    for halo_turn in (False, True):
        found = gathered(
            bounds, send, points, halo if halo_turn else None, embed_weight, embed_bias,
            halo_turn,
        )
        totals = node_sums(
            bounds, found, place, recv, edge_features, totals, pieces, rows, columns, mesh_nodes, halo_turn,
        )
    return finished(
        totals, recv, message_bias, pieces, rows, mesh_nodes
    )


def solution(mesh):
    return jax.shard_map(
        on_device,
        mesh=mesh,
        in_specs=(
            P("lon", None),
            P(),
            P(),
            P("lon", "ch"),
            P(None, "lon"),
            P("lon"),
            P("lon"),
            P(None, "ch"),
            P(None, "ch"),
            P(None, "ch"),
            P("ch"),
            P("ch", None),
            P(),
            P("ch"),
            P("ch"),
        ),
        out_specs=P("lon", "ch"),
        check_vma=False,
    )
```

```python
import functools

import jax
import jax.numpy as jnp
from jax import lax
from jax.experimental import pallas as pl
from jax.experimental.pallas import tpu as pltpu
from jax.sharding import PartitionSpec as P


LAT = 640
HALO = 4
UNIT = 512
WINDOW = 7
SLOTS = 8
PARTS = 4
LANES = 128
CHUNK = 256


def silu_of_double(half):
    return half + half * jnp.tanh(half)


def turn_units(units, ch_count):
    return -(-units * 5 // (8 * ch_count))


def low_of(bounds_ref, u):
    return bounds_ref[0, u * (UNIT // LANES)]


def high_of(bounds_ref, u):
    return bounds_ref[1, u * (UNIT // LANES)]


def pick_units(bounds_ref, list_ref, units, columns, halo_turn):
    me = lax.axis_index("ch")
    ch_count = lax.axis_size("ch")
    one = lambda flag: jnp.where(flag, 1, 0)
    at_left = [one(low_of(bounds_ref, u) < HALO) for u in range(units)]
    at_right = [one(high_of(bounds_ref, u) >= HALO + columns) for u in range(units)]
    lefts, rights = sum(at_left), sum(at_right)
    inner_count = units - lefts - rights
    end_share = -(-units // ch_count)
    first = jnp.minimum(jnp.maximum(end_share - lefts, 0), inner_count)
    last = jnp.maximum(inner_count - jnp.maximum(end_share - rights, 0), first)
    middle = lambda k: first + lax.div((last - first) * (k - 1), ch_count - 2)
    begin = jnp.where(me == 0, 0, middle(me))
    end = jnp.where(me == ch_count - 1, inner_count, middle(me + 1))
    first_turn = turn_units(units, ch_count)
    count, rank = jnp.int32(0), jnp.int32(0)
    for u in range(units):
        inner = 1 - at_left[u] - at_right[u]
        if halo_turn:
            inside = jnp.logical_and(rank >= begin + first_turn, rank < end)
            at_mine = jnp.where(me == 0, at_left[u], 0) + jnp.where(
                me == ch_count - 1, at_right[u], 0
            )
            mine = jnp.where(inside, inner, at_mine)
        else:
            inside = jnp.logical_and(
                rank >= begin, rank < jnp.minimum(begin + first_turn, end)
            )
            mine = jnp.where(inside, inner, 0)
        list_ref[count] = u
        count = count + mine
        rank = rank + inner
    return count


def spread(ref, ids):
    for n in range(ids.shape[0] // 8):
        tile = ids[8 * n:8 * n + 8]
        ref[16 * n:16 * n + 8, :] = tile
        ref[16 * n + 8:16 * n + 16, :] = pltpu.roll(tile, 4, 0)


def prepare_kernel(
    columns,
    x_ref,
    *refs,
):
    sources, refs = refs[:10], refs[10:]
    (edge_ref, packed_ref, send_ref, recv_ref, place_ref, bounds_ref, buffer, packed,
     senders_ref, receivers_ref, feature_ref, bias_ref, gain_ref, shift_ref,
     in_sem, out_sem, pack_sem, source_sem) = refs
    lon_count = lax.axis_size("lon")
    lon_place, ch_place = lax.axis_index("lon"), lax.axis_index("ch")
    start = jnp.where(ch_place == 0, (columns - HALO) * LAT, 0)
    takes = [
        pltpu.make_async_copy(
            x_ref.at[:, pl.ds(pl.multiple_of(start + n * LAT, LANES), LAT)],
            buffer.at[n],
            in_sem.at[n],
        )
        for n in range(HALO)
    ]
    gives = [
        pltpu.make_async_copy(
            buffer.at[n], edge_ref.at[:, pl.ds(n * LAT, LAT)], out_sem.at[n]
        )
        for n in range(HALO)
    ]
    targets = [senders_ref, receivers_ref]
    row = 0
    for ref in sources[2:5]:
        targets.append(packed.at[pl.ds(row, ref.shape[0]), :])
        row += ref.shape[0]
    targets += [feature_ref, bias_ref, gain_ref, shift_ref]
    loads = [
        pltpu.make_async_copy(source, target, source_sem.at[n])
        for n, (source, target) in enumerate(zip(sources, targets))
    ]
    tall, part = sources[9].shape[0], packed.shape[1]
    loads += [
        pltpu.make_async_copy(
            sources[9].at[:, pl.ds(n * part, part)],
            packed.at[pl.ds(row + 16 + n * tall, tall), :],
            source_sem.at[9 + n],
        )
        for n in range(sources[9].shape[1] // part)
    ]
    for copy in takes + loads:
        copy.start()
    for take, give in zip(takes, gives):
        take.wait()
        give.start()
    for copy in loads:
        copy.wait()
    singles = [feature_ref[...].astype(jnp.float32)]
    for ref in (bias_ref, gain_ref, shift_ref):
        rest = ref[...]
        for _ in range(3):
            high = rest.astype(jnp.bfloat16).astype(jnp.float32)
            singles.append(high)
            rest = rest - high
    used = feature_ref.shape[0] + len(singles) - 1
    singles.append(jnp.zeros((16 - used, singles[0].shape[1]), jnp.float32))
    packed[row:row + 16, :] = jnp.concatenate(singles).astype(jnp.bfloat16)
    pack = pltpu.make_async_copy(packed, packed_ref, pack_sem)
    pack.start()

    senders = senders_ref[...]
    column = lax.shift_right_logical(
        lax.shift_right_logical(senders, 7) * 52429, 18
    )
    latitude = senders - column * LAT
    total = columns * lon_count
    column = column - lon_place * columns + HALO
    column = jnp.where(column < 0, column + total, column)
    column = jnp.where(column >= total, column - total, column)
    parts = PARTS
    spread(send_ref, (jnp.bitwise_and(column, SLOTS - 1) * LAT + latitude) * parts)
    recv = receivers_ref[...] - lon_place * sources[4].shape[0]
    recv_ref[...] = recv
    spread(place_ref, recv * parts)
    tall = -(-senders.shape[0] // LANES) * LANES
    for n, (pick, near, fill) in enumerate(
        ((jnp.min, jnp.minimum, total), (jnp.max, jnp.maximum, 0))
    ):
        best = column
        for shift in (1, 2):
            best = near(best, pltpu.roll(best, best.shape[0] - shift, 0))
        best = jnp.concatenate(
            [best, jnp.full((tall - best.shape[0], LANES), fill, jnp.int32)]
        )
        bounds_ref[n:n + 1, :] = pick(jnp.transpose(best), axis=0, keepdims=True)
    for give in gives:
        give.wait()
    pack.wait()


def prepared(points, senders, receivers, sender_weight, receiver_weight, mesh_latent,
             feature_weight, hidden_bias, norm_gain, norm_shift, message_weight):
    columns = points.shape[1] // LAT
    assert LAT == 5 * LANES and lax.axis_size("lon") * points.shape[1] // LANES < 40960
    rows = senders.shape[0] // LANES
    part = sender_weight.shape[1]
    packed_rows = (
        2 * sender_weight.shape[0] + receiver_weight.shape[0] + mesh_latent.shape[0] + 16
    )
    vmem = pl.BlockSpec(memory_space=pltpu.VMEM)
    hbm = pl.BlockSpec(memory_space=pltpu.HBM)
    ids = jax.ShapeDtypeStruct((rows, LANES), jnp.int32)
    wide_ids = jax.ShapeDtypeStruct((2 * rows, LANES), jnp.int32)
    assert rows % 8 == 0 and UNIT == 4 * LANES
    return pl.pallas_call(
        functools.partial(prepare_kernel, columns),
        in_specs=[hbm] * 11,
        out_specs=[hbm, hbm, vmem, vmem, vmem, vmem],
        out_shape=[
            jax.ShapeDtypeStruct((points.shape[0], HALO * LAT), points.dtype),
            jax.ShapeDtypeStruct((packed_rows, part), jnp.bfloat16),
            wide_ids,
            ids,
            wide_ids,
            jax.ShapeDtypeStruct((2, -(-rows // LANES) * LANES), jnp.int32),
        ],
        scratch_shapes=[
            pltpu.VMEM((HALO, points.shape[0], LAT), points.dtype),
            pltpu.VMEM((packed_rows, part), jnp.bfloat16),
            pltpu.VMEM((rows, LANES), jnp.int32),
            pltpu.VMEM((rows, LANES), jnp.int32),
            pltpu.VMEM(feature_weight.shape, jnp.bfloat16),
            pltpu.VMEM((1, part), jnp.float32),
            pltpu.VMEM((1, part), jnp.float32),
            pltpu.VMEM((1, part), jnp.float32),
            pltpu.SemaphoreType.DMA((HALO,)),
            pltpu.SemaphoreType.DMA((HALO,)),
            pltpu.SemaphoreType.DMA,
            pltpu.SemaphoreType.DMA((9 + PARTS,)),
        ],
        compiler_params=pltpu.CompilerParams(vmem_limit_bytes=63 << 20),
    )(points, senders.reshape(rows, LANES), receivers.reshape(rows, LANES), sender_weight,
      receiver_weight, mesh_latent, feature_weight, hidden_bias.reshape(1, -1),
      norm_gain.reshape(1, -1), norm_shift.reshape(1, -1), message_weight)


def index_rows(u):
    return pl.ds(pl.multiple_of(u * 8, 8), 8)


def point_scratch(units, channels, width):
    parts = width // LANES
    return [
        pltpu.SMEM((units + 1,), jnp.int32),
        pltpu.SMEM((units * WINDOW + 1,), jnp.int32),
        pltpu.SMEM((units + 1,), jnp.int32),
        pltpu.SMEM((SLOTS,), jnp.int32),
        pltpu.SMEM((8, LANES), jnp.int32),
        pltpu.SMEM((8, LANES), jnp.int32),
        pltpu.VMEM((6, channels, LAT), jnp.bfloat16),
        pltpu.VMEM((SLOTS * LAT * parts, LANES), jnp.float32),
        pltpu.VMEM((CHUNK * parts, LANES), jnp.float32),
        pltpu.VMEM((CHUNK * parts, LANES), jnp.float32),
        pltpu.VMEM((channels, width), jnp.bfloat16),
        pltpu.VMEM((1, width), jnp.float32),
        pltpu.SemaphoreType.DMA((2,)),
        pltpu.SemaphoreType.DMA((6,)),
        pltpu.SemaphoreType.DMA((2,)),
    ]


POINT_SCRATCH = 15


def point_tools(columns, later, bounds_ref, send_ref, x_ref, halo_ref, embed_ref, bias_ref,
                scratch):
    (list_ref, events, event_at, held_column, index_even, index_odd, points, table, even, odd,
     embed_half, bias_half, index_sem, point_sem, weight_sem) = scratch
    index = (index_even, index_odd)
    parts = embed_half.shape[1] // LANES
    step = LAT * parts
    depth = points.shape[0]
    weights = [
        pltpu.make_async_copy(source, target, weight_sem.at[n])
        for n, (source, target) in enumerate(((embed_ref, embed_half), (bias_ref, bias_half)))
    ]
    for copy in weights:
        copy.start()
    count = pick_units(bounds_ref, list_ref, list_ref.shape[0] - 1, columns, later)

    for n in range(SLOTS):
        held_column[n] = -1

    def note_unit(n, total):
        u = list_ref[n]
        event_at[n] = total

        def note(column, total):
            slot = lax.rem(column, SLOTS)
            new = jnp.where(held_column[slot] == column, 0, 1)
            held_column[slot] = column
            events[total] = column
            return total + new

        return lax.fori_loop(low_of(bounds_ref, u), high_of(bounds_ref, u) + 1, note, total)

    total = lax.fori_loop(0, count, note_unit, jnp.int32(0))
    event_at[count] = total

    def fetch(event):
        column, slot = events[event], lax.rem(event, depth)

        def copy(source, place):
            start = pl.multiple_of(place * LAT, LANES)
            return pltpu.make_async_copy(
                source.at[:, pl.ds(start, LAT)], points.at[slot], point_sem.at[slot]
            )

        if not later:
            copy(x_ref, column - HALO).start()
            return
        last = column >= HALO + columns
        outside = jnp.logical_or(column < HALO, last)
        pl.when(outside)(
            lambda: copy(halo_ref, jnp.where(last, column - HALO - columns, column)).start()
        )
        pl.when(jnp.logical_not(outside))(lambda: copy(x_ref, column - HALO).start())

    def index_copy(n, turn):
        return pltpu.make_async_copy(
            send_ref.at[index_rows(list_ref[n]), :], index[turn], index_sem.at[turn]
        )

    def fetch_first(event, carry):
        fetch(event)
        return carry

    lax.fori_loop(0, jnp.minimum(total, depth), fetch_first, 0)
    for n in range(2):
        pl.when(n < count)(lambda n=n: index_copy(n, n).start())
    for copy in weights:
        copy.wait()
    embed_half[...] = embed_half[...] * jnp.bfloat16(0.5)
    bias_half[...] = bias_half[...] * 0.5

    def one_event(event, carry):
        slot = lax.rem(event, depth)
        pltpu.make_async_copy(
            x_ref.at[:, pl.ds(0, LAT)], points.at[slot], point_sem.at[slot]
        ).wait()
        before = lax.dot_general(
            points[slot], embed_half[...], (((0,), (0,)), ((), ())),
            preferred_element_type=jnp.float32,
        ) + bias_half[...]
        latent = silu_of_double(before)
        base = lax.rem(events[event], SLOTS) * step
        for j in range(parts):
            table[pl.ds(base + j, LAT, stride=parts), :] = latent[:, j * LANES:(j + 1) * LANES]
        pl.when(event + depth < total)(lambda: fetch(event + depth))
        return carry

    def bring(n, turn):
        lax.fori_loop(event_at[n], event_at[n + 1], one_event, 0)
        index_copy(n, turn).wait()

    def gather(turn, half):
        held = (even, odd)[half]
        row = half * (CHUNK // LANES)
        for i in range(CHUNK):
            place = pl.multiple_of(index[turn][row + i // LANES, i % LANES], parts)
            held[pl.ds(parts * i, parts), :] = table[pl.ds(place, parts), :]

    def leave(half, target, start):
        held = (even, odd)[half]
        for j in range(parts):
            target[pl.ds(start, CHUNK), j * LANES:(j + 1) * LANES] = (
                held[pl.ds(j, CHUNK, stride=parts), :].astype(jnp.bfloat16)
            )

    def next_index(n, turn):
        pl.when(n + 2 < count)(lambda: index_copy(n + 2, turn).start())

    return count, list_ref, bring, gather, leave, next_index


def gather_kernel(columns, bounds_ref, send_ref, x_ref, embed_ref, bias_ref, out_ref, *scratch):
    count, _, bring, gather, leave, next_index = point_tools(
        columns, False, bounds_ref, send_ref, x_ref, None, embed_ref, bias_ref, scratch
    )
    spare = out_ref.shape[0] - CHUNK

    def second_half(n):
        place = jnp.where(n > 0, (n - 1) * UNIT + CHUNK, spare)
        return pl.multiple_of(place, CHUNK)

    def one_unit(n, turn):
        bring(n, turn)
        leave(1, out_ref, second_half(n))
        gather(turn, 0)
        leave(0, out_ref, pl.multiple_of(n * UNIT, UNIT))
        gather(turn, 1)
        next_index(n, turn)

    def two_units(m, carry):
        one_unit(2 * m, 0)
        pl.when(2 * m + 1 < count)(lambda: one_unit(2 * m + 1, 1))
        return carry

    lax.fori_loop(0, (count + 1) // 2, two_units, 0)
    pl.when(count > 0)(lambda: leave(1, out_ref, second_half(count)))


def gathered(bounds, send, points, embed_weight, embed_bias):
    channels, width = embed_weight.shape
    columns = points.shape[1] // LAT
    units = send.shape[0] // 8
    most = turn_units(units, lax.axis_size("ch"))
    vmem = pl.BlockSpec(memory_space=pltpu.VMEM)
    smem = pl.BlockSpec(memory_space=pltpu.SMEM)
    hbm = pl.BlockSpec(memory_space=pltpu.HBM)
    return pl.pallas_call(
        functools.partial(gather_kernel, columns),
        in_specs=[smem, hbm, hbm, hbm, hbm],
        out_specs=vmem,
        out_shape=jax.ShapeDtypeStruct((most * UNIT + CHUNK, width), jnp.bfloat16),
        scratch_shapes=point_scratch(units, channels, width),
        compiler_params=pltpu.CompilerParams(vmem_limit_bytes=40 << 20),
        cost_estimate=pl.CostEstimate(
            flops=2 * units * UNIT * channels * width,
            bytes_accessed=units * UNIT * width,
            transcendentals=units * UNIT * width // 2,
        ),
    )(bounds, send, points, embed_weight, embed_bias.reshape(1, -1))


def sum_tools(list_ref, features_ref, recv_ref, sender_all, feature_all, hidden, out_ref):
    nodes, width = out_ref.shape
    parts = width // LANES
    components = features_ref.shape[0]

    def activate(n, turn, rows, terms):
        start = pl.multiple_of(list_ref[n] * UNIT, UNIT)
        mine = slice(turn * UNIT, (turn + 1) * UNIT)
        before = jnp.dot(rows, sender_all[...], preferred_element_type=jnp.float32)
        before += lax.dot_general(
            features_ref[:, pl.ds(start, UNIT)], feature_all[:components, :],
            (((0,), (0,)), ((), ())),
            preferred_element_type=jnp.float32,
        )
        for j in range(parts):
            lanes = slice(j * LANES, (j + 1) * LANES)
            hidden[mine, lanes] = silu_of_double(
                before[:, lanes] + terms[pl.ds(j, UNIT, stride=parts), :]
            ).astype(jnp.bfloat16)

    def add_up(first, turn, number, live=True):
        each = lax.broadcasted_iota(jnp.int32, (nodes, LANES), 0)
        blocks = []
        for n in range(number):
            for b in range(UNIT // LANES):
                ids = recv_ref[pl.ds(list_ref[first + n] * (UNIT // LANES) + b, 1), :]
                ids = ids if live is True else jnp.where(live, ids, -1)
                blocks.append(jnp.where(each == ids, 1.0, 0.0))
        by_node = jnp.concatenate(blocks, axis=1).astype(jnp.bfloat16)
        mine = slice(turn * UNIT, (turn + number) * UNIT)
        out_ref[...] += jnp.dot(by_node, hidden[mine, :], preferred_element_type=jnp.float32)

    return activate, add_up


def edge_kernel(
    columns,
    rows,
    bounds_ref,
    found_ref,
    place_ref,
    recv_ref,
    features_ref,
    *refs,
):
    ways = lax.axis_size("ch")
    pieces = refs[:ways]
    (out_ref, sender_all, recv_terms, feature_all, list_ref, index, receiver_all, even, odd,
     hidden, index_sem) = refs[ways:]
    me = lax.axis_index("ch")
    nodes, width = out_ref.shape
    part = width // ways
    parts = width // LANES
    rings = index.shape[0]
    count = pick_units(bounds_ref, list_ref, list_ref.shape[0] - 1, columns, False)
    activate, add_up = sum_tools(
        list_ref, features_ref, recv_ref, sender_all, feature_all, hidden, out_ref
    )

    def fetch_index(n):
        slot = lax.rem(n, rings)
        return pltpu.make_async_copy(
            place_ref.at[index_rows(list_ref[n]), :], index.at[slot], index_sem.at[slot]
        )

    for n in range(rings - 2):
        pl.when(n < count)(lambda n=n: fetch_index(n).start())
    at = [sum(rows[:n]) for n in range(len(rows) + 1)]
    for j, piece in enumerate(pieces):
        lanes = slice(j * part, (j + 1) * part)
        sender_all[:, lanes] = piece[at[0]:at[1], :] * jnp.bfloat16(0.5)
        receiver_all[:, lanes] = piece[at[1]:at[2], :]
        feature_all[:, lanes] = piece[at[3]:at[4], :] * jnp.bfloat16(0.5)
    components = features_ref.shape[0]
    singles = jnp.concatenate([piece[at[3]:at[4], :] for piece in pieces], axis=1)
    singles = singles.astype(jnp.float32)
    terms = jnp.broadcast_to(
        singles[components:components + 1] + singles[components + 1:components + 2]
        + singles[components + 2:components + 3],
        (nodes, width),
    )
    for j, piece in enumerate(pieces):
        owner = jnp.bitwise_xor(me, j)
        terms += jnp.dot(
            piece[at[2]:at[3], :],
            receiver_all[pl.ds(pl.multiple_of(owner * part, part), part), :],
            preferred_element_type=jnp.float32,
        )
    for j in range(parts):
        recv_terms[pl.ds(j, nodes, stride=parts), :] = (
            0.5 * terms[:, j * LANES:(j + 1) * LANES]
        )
    out_ref[...] = jnp.zeros_like(out_ref)

    def gather(n, held):
        slot = lax.rem(n, rings)
        for i in range(UNIT):
            place = pl.multiple_of(index[slot, i // LANES, i % LANES], parts)
            held[pl.ds(parts * i, parts), :] = recv_terms[pl.ds(place, parts), :]

    def found(n):
        return found_ref[pl.ds(pl.multiple_of(n * UNIT, UNIT), UNIT), :]

    @pl.when(count > 0)
    def _():
        fetch_index(0).wait()
        gather(0, even)

    def pair(m, carry):
        first, second = 2 * m, 2 * m + 1
        after = second + 1 < count
        for n in (first, second):
            pl.when(n + rings - 2 < count)(lambda n=n: fetch_index(n + rings - 2).start())
        fetch_index(second).wait()
        gather(second, odd)
        activate(first, 0, found(first), even)
        pl.when(after)(lambda: fetch_index(second + 1).wait())
        gather(jnp.where(after, second + 1, second), even)
        activate(second, 1, found(second), odd)
        add_up(first, 0, 2)
        return carry

    lax.fori_loop(0, count // 2, pair, 0)

    @pl.when(lax.rem(count, 2) == 1)
    def _():
        activate(count - 1, 0, found(count - 1), even)
        add_up(count - 1, 0, 1)


def first_sums(bounds, found, place, recv, features, pieces, rows, columns, nodes):
    width = found.shape[1]
    units = place.shape[0] // 8
    parts = width // LANES
    vmem = pl.BlockSpec(memory_space=pltpu.VMEM)
    smem = pl.BlockSpec(memory_space=pltpu.SMEM)
    hbm = pl.BlockSpec(memory_space=pltpu.HBM)
    edges = found.shape[0]
    return pl.pallas_call(
        functools.partial(edge_kernel, columns, rows),
        in_specs=[smem, vmem, hbm, vmem, vmem] + [vmem] * len(pieces),
        out_specs=[vmem] * 4,
        out_shape=[
            jax.ShapeDtypeStruct((nodes, width), jnp.float32),
            jax.ShapeDtypeStruct((width, width), jnp.bfloat16),
            jax.ShapeDtypeStruct((nodes * parts, LANES), jnp.float32),
            jax.ShapeDtypeStruct((rows[3], width), jnp.bfloat16),
        ],
        scratch_shapes=[
            pltpu.SMEM((units + 1,), jnp.int32),
            pltpu.SMEM((6, 8, LANES), jnp.int32),
            pltpu.VMEM((width, width), jnp.bfloat16),
            pltpu.VMEM((UNIT * parts, LANES), jnp.float32),
            pltpu.VMEM((UNIT * parts, LANES), jnp.float32),
            pltpu.VMEM((2 * UNIT, width), jnp.bfloat16),
            pltpu.SemaphoreType.DMA((6,)),
        ],
        compiler_params=pltpu.CompilerParams(vmem_limit_bytes=40 << 20),
        cost_estimate=pl.CostEstimate(
            flops=2 * edges * width * (width + nodes),
            bytes_accessed=edges * width,
            transcendentals=edges * width,
        ),
    )(bounds, found, place, recv, features, *pieces)


def later_kernel(
    columns,
    bounds_ref,
    send_ref,
    x_ref,
    halo_ref,
    embed_ref,
    bias_ref,
    place_ref,
    recv_ref,
    features_ref,
    start_ref,
    sender_all,
    recv_terms,
    feature_all,
    out_ref,
    *refs,
):
    scratch = refs[:POINT_SCRATCH]
    (place_even, place_odd, rows_even, rows_odd, terms_even, terms_odd, hidden,
     place_sem) = refs[POINT_SCRATCH:]
    parts = out_ref.shape[1] // LANES
    places, rows, terms = (
        (place_even, place_odd), (rows_even, rows_odd), (terms_even, terms_odd)
    )
    count, list_ref, bring, gather, leave, next_index = point_tools(
        columns, True, bounds_ref, send_ref, x_ref, halo_ref, embed_ref, bias_ref, scratch
    )
    activate, add_up = sum_tools(
        list_ref, features_ref, recv_ref, sender_all, feature_all, hidden, out_ref
    )

    def place_copy(n, turn):
        return pltpu.make_async_copy(
            place_ref.at[index_rows(list_ref[n]), :], places[turn], place_sem.at[turn]
        )

    for n in range(2):
        pl.when(n < count)(lambda n=n: place_copy(n, n).start())
    out_ref[...] = start_ref[...]
    rows_odd[...] = jnp.zeros_like(rows_odd)
    terms_odd[...] = jnp.zeros_like(terms_odd)

    def gather_terms(turn):
        for i in range(UNIT):
            place = pl.multiple_of(places[turn][i // LANES, i % LANES], parts)
            terms[turn][pl.ds(parts * i, parts), :] = recv_terms[pl.ds(place, parts), :]

    def one_unit(n, turn):
        bring(n, turn)
        place_copy(n, turn).wait()
        gather(turn, 0)
        gather(turn, 1)
        before = jnp.maximum(n - 1, 0)
        activate(before, 0, rows[1 - turn][...], terms[1 - turn])
        leave(0, rows[turn], 0)
        leave(1, rows[turn], CHUNK)
        gather_terms(turn)
        add_up(before, 0, 1, n > 0)
        next_index(n, turn)
        pl.when(n + 2 < count)(lambda: place_copy(n + 2, turn).start())

    def two_units(m, carry):
        one_unit(2 * m, 0)
        pl.when(2 * m + 1 < count)(lambda: one_unit(2 * m + 1, 1))
        return carry

    lax.fori_loop(0, (count + 1) // 2, two_units, 0)
    for turn in range(2):
        @pl.when(jnp.logical_and(count > 0, lax.rem(count - 1, 2) == turn))
        def _(turn=turn):
            activate(count - 1, 0, rows[turn][...], terms[turn])
            add_up(count - 1, 0, 1)


def later_sums(bounds, send, points, halo, embed_weight, embed_bias, place, recv, features,
               start, sender_all, recv_terms, feature_all):
    channels, width = embed_weight.shape
    columns = points.shape[1] // LAT
    units = send.shape[0] // 8
    parts = width // LANES
    vmem = pl.BlockSpec(memory_space=pltpu.VMEM)
    smem = pl.BlockSpec(memory_space=pltpu.SMEM)
    hbm = pl.BlockSpec(memory_space=pltpu.HBM)
    return pl.pallas_call(
        functools.partial(later_kernel, columns),
        in_specs=[smem] + [hbm] * 6 + [vmem] * 6,
        out_specs=vmem,
        out_shape=jax.ShapeDtypeStruct(start.shape, jnp.float32),
        scratch_shapes=point_scratch(units, channels, width) + [
            pltpu.SMEM((8, LANES), jnp.int32),
            pltpu.SMEM((8, LANES), jnp.int32),
            pltpu.VMEM((UNIT, width), jnp.bfloat16),
            pltpu.VMEM((UNIT, width), jnp.bfloat16),
            pltpu.VMEM((UNIT * parts, LANES), jnp.float32),
            pltpu.VMEM((UNIT * parts, LANES), jnp.float32),
            pltpu.VMEM((UNIT, width), jnp.bfloat16),
            pltpu.SemaphoreType.DMA((2,)),
        ],
        compiler_params=pltpu.CompilerParams(vmem_limit_bytes=40 << 20),
        cost_estimate=pl.CostEstimate(
            flops=units * UNIT * width * (channels + width),
            bytes_accessed=units * UNIT * width,
            transcendentals=units * UNIT * width,
        ),
    )(bounds, send, points, halo, embed_weight, embed_bias.reshape(1, -1), place, recv,
      features, start, sender_all, recv_terms, feature_all)


def swap_kernel(own_ref, far_ref, own_out, far_out, send, recv):
    beside = across(lax.axis_index("ch"), 1)
    barrier = pltpu.get_barrier_semaphore()
    pl.semaphore_signal(
        barrier, inc=1, device_id={"ch": beside}, device_id_type=pl.DeviceIdType.MESH
    )
    pl.semaphore_wait(barrier, 1)
    copies = [
        pltpu.make_async_remote_copy(
            src_ref=source, dst_ref=target, send_sem=send.at[n], recv_sem=recv.at[n],
            device_id={"ch": beside}, device_id_type=pl.DeviceIdType.MESH,
        )
        for n, (source, target) in enumerate(((own_ref, own_out), (far_ref, far_out)))
    ]
    for copy in copies:
        copy.start()
    for copy in copies:
        copy.wait()


def swapped_beside(own, far):
    vmem = pl.BlockSpec(memory_space=pltpu.VMEM)
    return pl.pallas_call(
        swap_kernel,
        in_specs=[vmem] * 2,
        out_specs=[vmem] * 2,
        out_shape=[jax.ShapeDtypeStruct(own.shape, own.dtype)] * 2,
        scratch_shapes=[pltpu.SemaphoreType.DMA((2,)), pltpu.SemaphoreType.DMA((2,))],
        compiler_params=pltpu.CompilerParams(
            vmem_limit_bytes=8 << 20, collective_id=0, has_side_effects=True
        ),
    )(own, far)


def across(me, bit):
    return me + bit - 2 * bit * lax.rem(me // bit, 2)


def swapped(block, bit, width):
    parts = block.shape[1] // width
    return jnp.concatenate(
        [block[:, (n ^ bit) * width:((n ^ bit) + 1) * width] for n in range(parts)], axis=1
    )


def tail_kernel(
    rows,
    totals_ref,
    recv_ref,
    message_bias_ref,
    *refs,
):
    ch_count = lax.axis_size("ch")
    pieces = refs[:ch_count]
    (out_ref, near, onward, far, normed, give, near_send, near_recv, far_send, far_recv,
     back_send, back_recv, messages) = refs[ch_count:]
    me = lax.axis_index("ch")
    parts, part, width = normed.shape
    beside, opposite = across(me, 1), across(me, 2)
    partners = [beside, opposite, across(opposite, 1)]
    barrier = pltpu.get_barrier_semaphore()
    for partner in partners:
        pl.semaphore_signal(
            barrier, inc=1, device_id={"ch": partner}, device_id_type=pl.DeviceIdType.MESH
        )
    pl.semaphore_wait(barrier, ch_count - 1)

    def copy_to(source, target, send, recv, partner):
        return pltpu.make_async_remote_copy(
            src_ref=source, dst_ref=target, send_sem=send, recv_sem=recv,
            device_id={"ch": partner}, device_id_type=pl.DeviceIdType.MESH,
        )

    half = part // 2
    halves = [pl.ds(n * half, half) for n in range(2)]
    nears = [
        copy_to(
            totals_ref.at[partners[2], some, :], near.at[0, some, :], near_send.at[n],
            near_recv.at[n], beside,
        )
        for n, some in enumerate(halves)
    ]
    nears.append(
        copy_to(totals_ref.at[beside], near.at[1], near_send.at[2], near_recv.at[2], beside)
    )
    for copy in nears:
        copy.start()
    at = [sum(rows[:n]) for n in range(len(rows) + 1)]
    for n in range(parts):
        for j in range(parts):
            first = at[4] + j * width
            messages[n, :, j * width:(j + 1) * width] = pieces[n][first:first + width, :]
    pass_on = []
    for n, some in enumerate(halves):
        nears[n].wait()
        onward[some, :] = (
            totals_ref[opposite, some, :] + swapped(near[0, some, :], 1, width)
        ).astype(onward.dtype)
        pass_on.append(
            copy_to(
                onward.at[some, :], far.at[some, :], far_send.at[n], far_recv.at[n], opposite
            )
        )
        pass_on[n].start()

    def tally(n, counts):
        nodes_here = lax.broadcasted_iota(jnp.int32, (part, LANES), 0) + me * part
        for i in range(8):
            ids = recv_ref[pl.ds(n * 8 + i, 1), :]
            counts = counts + jnp.where(nodes_here == ids, 1.0, 0.0)
        return counts

    counts = lax.fori_loop(
        0, recv_ref.shape[0] // 8, tally, jnp.zeros((part, LANES), jnp.float32)
    )
    aggregated = jnp.sum(counts, axis=1, keepdims=True) * message_bias_ref[...]
    nears[2].wait()
    sums = totals_ref[me] + swapped(near[1], 1, width)
    for copy in pass_on:
        copy.wait()
    sums = sums + swapped(far[...].astype(jnp.float32), 2, width)
    for n in range(parts):
        rest = sums[:, n * width:(n + 1) * width]
        for _ in range(2):
            piece = rest.astype(jnp.bfloat16)
            aggregated += jnp.dot(
                piece, messages[n], preferred_element_type=jnp.float32
            )
            rest = rest - piece.astype(jnp.float32)
    centre = jnp.mean(aggregated, axis=1, keepdims=True)
    spread = jnp.mean(jnp.square(aggregated - centre), axis=1, keepdims=True)
    result = (aggregated - centre) * lax.rsqrt(spread + 1.0)
    for n in range(parts):
        normed[n] = result[:, n * width:(n + 1) * width]
    mine = pl.ds(pl.multiple_of(me * part, part), part)
    returns = []
    for j in (3, 2, 1, 0):
        owner = ([me] + partners)[j]
        small = pieces[j][at[3]:at[4], :].astype(jnp.float32)
        gain = small[7:8] + small[8:9] + small[9:10]
        shift = small[10:11] + small[11:12] + small[12:13]
        latent = pieces[j][pl.ds(at[2] + pl.multiple_of(me * part, part), part), :]
        block = (latent.astype(jnp.float32) + normed[owner] * gain + shift).astype(out_ref.dtype)
        if j == 0:
            out_ref[mine, :] = block
            continue
        give[j - 1] = block
        copy = copy_to(
            give.at[j - 1], out_ref.at[mine, :], back_send.at[j - 1], back_recv.at[j - 1], owner
        )
        copy.start()
        returns.append(copy)
    for copy in returns:
        copy.wait()


def finished(totals, recv, message_bias, pieces, rows, nodes):
    ch_count = lax.axis_size("ch")
    part = nodes // ch_count
    full = totals.shape[1]
    width = full // ch_count
    vmem = pl.BlockSpec(memory_space=pltpu.VMEM)
    return pl.pallas_call(
        functools.partial(tail_kernel, rows),
        in_specs=[vmem] * (3 + ch_count),
        out_specs=vmem,
        out_shape=jax.ShapeDtypeStruct((nodes, width), jnp.bfloat16),
        scratch_shapes=[
            pltpu.VMEM((2, part, full), jnp.float32),
            pltpu.VMEM((part, full), jnp.bfloat16),
            pltpu.VMEM((part, full), jnp.bfloat16),
            pltpu.VMEM((ch_count, part, width), jnp.float32),
            pltpu.VMEM((ch_count - 1, part, width), jnp.bfloat16),
            pltpu.SemaphoreType.DMA((3,)),
            pltpu.SemaphoreType.DMA((3,)),
            pltpu.SemaphoreType.DMA((2,)),
            pltpu.SemaphoreType.DMA((2,)),
            pltpu.SemaphoreType.DMA((ch_count - 1,)),
            pltpu.SemaphoreType.DMA((ch_count - 1,)),
            pltpu.VMEM((ch_count, width, full), jnp.bfloat16),
        ],
        compiler_params=pltpu.CompilerParams(
            vmem_limit_bytes=32 << 20, collective_id=1, has_side_effects=True
        ),
    )(totals.reshape(ch_count, part, full), recv, message_bias.reshape(1, -1), *pieces)


def on_device(
    grid_inputs,
    embed_weight,
    embed_bias,
    mesh_latent,
    edge_features,
    senders,
    receivers,
    sender_weight,
    receiver_weight,
    feature_weight,
    hidden_bias,
    message_weight,
    message_bias,
    norm_gain,
    norm_shift,
):
    lon_count, ch_count = lax.axis_size("lon"), lax.axis_size("ch")
    assert ch_count == 4
    columns = grid_inputs.shape[0] // LAT
    assert columns >= WINDOW
    mesh_nodes = mesh_latent.shape[0]
    width = embed_weight.shape[1]
    assert width == PARTS * LANES
    edges = senders.shape[0]
    unit = UNIT
    assert edges % unit == 0 and unit == 2 * CHUNK
    points = grid_inputs.T

    edge_columns, packed, send, recv, place, bounds = prepared(
        points, senders, receivers, sender_weight, receiver_weight, mesh_latent,
        feature_weight, hidden_bias, norm_gain, norm_shift, message_weight,
    )
    rows = (width, width, mesh_nodes, 16)
    hops = []
    for i in range(lon_count):
        hops.append((i * ch_count, (i + 1) % lon_count * ch_count))
        hops.append(
            (i * ch_count + ch_count - 1, (i - 1) % lon_count * ch_count + ch_count - 1)
        )
    halo = lax.ppermute(edge_columns, ("lon", "ch"), hops)

    opposite = lax.ppermute(packed, "ch", [(i, i ^ 2) for i in range(ch_count)])
    beside, diagonal = swapped_beside(packed, opposite)
    pieces = [packed, beside, opposite, diagonal]

    found = gathered(bounds, send, points, embed_weight, embed_bias)
    totals, *prepared_weights = first_sums(
        bounds, found, place, recv, edge_features, pieces, rows, columns, mesh_nodes
    )
    totals = later_sums(
        bounds, send, points, halo, embed_weight, embed_bias, place, recv, edge_features,
        totals, *prepared_weights,
    )
    return finished(
        totals, recv, message_bias, pieces, rows, mesh_nodes
    )


def solution(mesh):
    return jax.shard_map(
        on_device,
        mesh=mesh,
        in_specs=(
            P("lon", None),
            P(),
            P(),
            P("lon", "ch"),
            P(None, "lon"),
            P("lon"),
            P("lon"),
            P(None, "ch"),
            P(None, "ch"),
            P(None, "ch"),
            P("ch"),
            P("ch", None),
            P(),
            P("ch"),
            P("ch"),
        ),
        out_specs=P("lon", "ch"),
        check_vma=False,
    )
```

```python
import functools

import jax
import jax.numpy as jnp
from jax import lax
from jax.experimental import pallas as pl
from jax.experimental.pallas import tpu as pltpu
from jax.sharding import PartitionSpec as P


LAT = 640
HALO = 4
UNIT = 512
WINDOW = 7
SLOTS = 8
PARTS = 4
LANES = 128
CHUNK = 256


def silu_of_double(half):
    return half + half * jnp.tanh(half)


def turn_units(units, ch_count):
    return -(-units * 5 // (8 * ch_count))


def low_of(bounds_ref, u):
    return bounds_ref[0, u * (UNIT // LANES)]


def high_of(bounds_ref, u):
    return bounds_ref[1, u * (UNIT // LANES)]


def pick_units(bounds_ref, list_ref, units, columns, halo_turn):
    me = lax.axis_index("ch")
    ch_count = lax.axis_size("ch")
    one = lambda flag: jnp.where(flag, 1, 0)
    at_left = [one(low_of(bounds_ref, u) < HALO) for u in range(units)]
    at_right = [one(high_of(bounds_ref, u) >= HALO + columns) for u in range(units)]
    lefts, rights = sum(at_left), sum(at_right)
    inner_count = units - lefts - rights
    end_share = -(-units // ch_count)
    first = jnp.minimum(jnp.maximum(end_share - lefts, 0), inner_count)
    last = jnp.maximum(inner_count - jnp.maximum(end_share - rights, 0), first)
    middle = lambda k: first + lax.div((last - first) * (k - 1), ch_count - 2)
    begin = jnp.where(me == 0, 0, middle(me))
    end = jnp.where(me == ch_count - 1, inner_count, middle(me + 1))
    first_turn = turn_units(units, ch_count)
    count, rank = jnp.int32(0), jnp.int32(0)
    for u in range(units):
        inner = 1 - at_left[u] - at_right[u]
        if halo_turn:
            inside = jnp.logical_and(rank >= begin + first_turn, rank < end)
            at_mine = jnp.where(me == 0, at_left[u], 0) + jnp.where(
                me == ch_count - 1, at_right[u], 0
            )
            mine = jnp.where(inside, inner, at_mine)
        else:
            inside = jnp.logical_and(
                rank >= begin, rank < jnp.minimum(begin + first_turn, end)
            )
            mine = jnp.where(inside, inner, 0)
        list_ref[count] = u
        count = count + mine
        rank = rank + inner
    return count


def spread(ref, ids):
    for n in range(ids.shape[0] // 8):
        tile = ids[8 * n:8 * n + 8]
        ref[16 * n:16 * n + 8, :] = tile
        ref[16 * n + 8:16 * n + 16, :] = pltpu.roll(tile, 4, 0)


def cut_kernel(columns, x_ref, edge_ref, buffer, in_sem, out_sem):
    start = jnp.where(lax.axis_index("ch") == 0, (columns - HALO) * LAT, 0)
    takes = [
        pltpu.make_async_copy(
            x_ref.at[:, pl.ds(pl.multiple_of(start + n * LAT, LANES), LAT)],
            buffer.at[n],
            in_sem.at[n],
        )
        for n in range(HALO)
    ]
    gives = [
        pltpu.make_async_copy(
            buffer.at[n], edge_ref.at[:, pl.ds(n * LAT, LAT)], out_sem.at[n]
        )
        for n in range(HALO)
    ]
    for take in takes:
        take.start()
    for take, give in zip(takes, gives):
        take.wait()
        give.start()
    for give in gives:
        give.wait()


def cut_columns(points):
    hbm = pl.BlockSpec(memory_space=pltpu.HBM)
    return pl.pallas_call(
        functools.partial(cut_kernel, points.shape[1] // LAT),
        in_specs=[hbm],
        out_specs=hbm,
        out_shape=jax.ShapeDtypeStruct((points.shape[0], HALO * LAT), points.dtype),
        scratch_shapes=[
            pltpu.VMEM((HALO, points.shape[0], LAT), points.dtype),
            pltpu.SemaphoreType.DMA((HALO,)),
            pltpu.SemaphoreType.DMA((HALO,)),
        ],
        compiler_params=pltpu.CompilerParams(vmem_limit_bytes=40 << 20),
    )(points)


def prepare_kernel(
    columns,
    *refs,
):
    sources, refs = refs[:10], refs[10:]
    (packed_ref, send_ref, recv_ref, place_ref, bounds_ref, packed,
     senders_ref, receivers_ref, feature_ref, bias_ref, gain_ref, shift_ref,
     pack_sem, source_sem) = refs
    lon_count, lon_place = lax.axis_size("lon"), lax.axis_index("lon")
    targets = [senders_ref, receivers_ref]
    row = 0
    for ref in sources[2:5]:
        targets.append(packed.at[pl.ds(row, ref.shape[0]), :])
        row += ref.shape[0]
    targets += [feature_ref, bias_ref, gain_ref, shift_ref]
    loads = [
        pltpu.make_async_copy(source, target, source_sem.at[n])
        for n, (source, target) in enumerate(zip(sources, targets))
    ]
    tall, part = sources[9].shape[0], packed.shape[1]
    loads += [
        pltpu.make_async_copy(
            sources[9].at[:, pl.ds(n * part, part)],
            packed.at[pl.ds(row + 16 + n * tall, tall), :],
            source_sem.at[9 + n],
        )
        for n in range(sources[9].shape[1] // part)
    ]
    for copy in loads:
        copy.start()
    for copy in loads:
        copy.wait()
    singles = [feature_ref[...].astype(jnp.float32)]
    for ref in (bias_ref, gain_ref, shift_ref):
        rest = ref[...]
        for _ in range(3):
            high = rest.astype(jnp.bfloat16).astype(jnp.float32)
            singles.append(high)
            rest = rest - high
    used = feature_ref.shape[0] + len(singles) - 1
    singles.append(jnp.zeros((16 - used, singles[0].shape[1]), jnp.float32))
    packed[row:row + 16, :] = jnp.concatenate(singles).astype(jnp.bfloat16)
    pack = pltpu.make_async_copy(packed, packed_ref, pack_sem)
    pack.start()

    senders = senders_ref[...]
    column = lax.shift_right_logical(
        lax.shift_right_logical(senders, 7) * 52429, 18
    )
    latitude = senders - column * LAT
    total = columns * lon_count
    column = column - lon_place * columns + HALO
    column = jnp.where(column < 0, column + total, column)
    column = jnp.where(column >= total, column - total, column)
    parts = PARTS
    spread(send_ref, (jnp.bitwise_and(column, SLOTS - 1) * LAT + latitude) * parts)
    recv = receivers_ref[...] - lon_place * sources[4].shape[0]
    recv_ref[...] = recv
    spread(place_ref, recv * parts)
    tall = -(-senders.shape[0] // LANES) * LANES
    for n, (pick, near, fill) in enumerate(
        ((jnp.min, jnp.minimum, total), (jnp.max, jnp.maximum, 0))
    ):
        best = column
        for shift in (1, 2):
            best = near(best, pltpu.roll(best, best.shape[0] - shift, 0))
        best = jnp.concatenate(
            [best, jnp.full((tall - best.shape[0], LANES), fill, jnp.int32)]
        )
        bounds_ref[n:n + 1, :] = pick(jnp.transpose(best), axis=0, keepdims=True)
    pack.wait()


def prepared(columns, senders, receivers, sender_weight, receiver_weight, mesh_latent,
             feature_weight, hidden_bias, norm_gain, norm_shift, message_weight):
    assert LAT == 5 * LANES and lax.axis_size("lon") * columns * LAT // LANES < 40960
    rows = senders.shape[0] // LANES
    part = sender_weight.shape[1]
    packed_rows = (
        2 * sender_weight.shape[0] + receiver_weight.shape[0] + mesh_latent.shape[0] + 16
    )
    vmem = pl.BlockSpec(memory_space=pltpu.VMEM)
    hbm = pl.BlockSpec(memory_space=pltpu.HBM)
    ids = jax.ShapeDtypeStruct((rows, LANES), jnp.int32)
    wide_ids = jax.ShapeDtypeStruct((2 * rows, LANES), jnp.int32)
    assert rows % 8 == 0 and UNIT == 4 * LANES
    return pl.pallas_call(
        functools.partial(prepare_kernel, columns),
        in_specs=[hbm] * 10,
        out_specs=[hbm, vmem, vmem, vmem, vmem],
        out_shape=[
            jax.ShapeDtypeStruct((packed_rows, part), jnp.bfloat16),
            wide_ids,
            ids,
            wide_ids,
            jax.ShapeDtypeStruct((2, -(-rows // LANES) * LANES), jnp.int32),
        ],
        scratch_shapes=[
            pltpu.VMEM((packed_rows, part), jnp.bfloat16),
            pltpu.VMEM((rows, LANES), jnp.int32),
            pltpu.VMEM((rows, LANES), jnp.int32),
            pltpu.VMEM(feature_weight.shape, jnp.bfloat16),
            pltpu.VMEM((1, part), jnp.float32),
            pltpu.VMEM((1, part), jnp.float32),
            pltpu.VMEM((1, part), jnp.float32),
            pltpu.SemaphoreType.DMA,
            pltpu.SemaphoreType.DMA((9 + PARTS,)),
        ],
        compiler_params=pltpu.CompilerParams(vmem_limit_bytes=40 << 20),
    )(senders.reshape(rows, LANES), receivers.reshape(rows, LANES), sender_weight,
      receiver_weight, mesh_latent, feature_weight, hidden_bias.reshape(1, -1),
      norm_gain.reshape(1, -1), norm_shift.reshape(1, -1), message_weight)


def index_rows(u):
    return pl.ds(pl.multiple_of(u * 8, 8), 8)


def point_scratch(units, channels, width):
    parts = width // LANES
    return [
        pltpu.SMEM((units + 1,), jnp.int32),
        pltpu.SMEM((units * WINDOW + 1,), jnp.int32),
        pltpu.SMEM((units + 1,), jnp.int32),
        pltpu.SMEM((SLOTS,), jnp.int32),
        pltpu.SMEM((8, LANES), jnp.int32),
        pltpu.SMEM((8, LANES), jnp.int32),
        pltpu.VMEM((6, channels, LAT), jnp.bfloat16),
        pltpu.VMEM((SLOTS * LAT * parts, LANES), jnp.float32),
        pltpu.VMEM((CHUNK * parts, LANES), jnp.float32),
        pltpu.VMEM((CHUNK * parts, LANES), jnp.float32),
        pltpu.VMEM((channels, width), jnp.bfloat16),
        pltpu.VMEM((1, width), jnp.float32),
        pltpu.SemaphoreType.DMA((2,)),
        pltpu.SemaphoreType.DMA((6,)),
        pltpu.SemaphoreType.DMA((2,)),
    ]


POINT_SCRATCH = 15


def point_tools(columns, later, bounds_ref, send_ref, x_ref, halo_ref, embed_ref, bias_ref,
                scratch):
    (list_ref, events, event_at, held_column, index_even, index_odd, points, table, even, odd,
     embed_half, bias_half, index_sem, point_sem, weight_sem) = scratch
    index = (index_even, index_odd)
    parts = embed_half.shape[1] // LANES
    step = LAT * parts
    depth = points.shape[0]
    weights = [
        pltpu.make_async_copy(source, target, weight_sem.at[n])
        for n, (source, target) in enumerate(((embed_ref, embed_half), (bias_ref, bias_half)))
    ]
    for copy in weights:
        copy.start()
    count = pick_units(bounds_ref, list_ref, list_ref.shape[0] - 1, columns, later)

    def fetch(event):
        bring_in(events[event], lax.rem(event, depth))

    def bring_in(column, slot):
        def copy(source, place):
            start = pl.multiple_of(place * LAT, LANES)
            return pltpu.make_async_copy(
                source.at[:, pl.ds(start, LAT)], points.at[slot], point_sem.at[slot]
            )

        if not later:
            copy(x_ref, column - HALO).start()
            return
        last = column >= HALO + columns
        outside = jnp.logical_or(column < HALO, last)
        pl.when(outside)(
            lambda: copy(halo_ref, jnp.where(last, column - HALO - columns, column)).start()
        )
        pl.when(jnp.logical_not(outside))(lambda: copy(x_ref, column - HALO).start())

    pl.when(count > 0)(lambda: bring_in(low_of(bounds_ref, list_ref[0]), 0))
    for n in range(SLOTS):
        held_column[n] = -1

    def note_unit(n, total):
        u = list_ref[n]
        event_at[n] = total

        def note(column, total):
            slot = lax.rem(column, SLOTS)
            new = jnp.where(held_column[slot] == column, 0, 1)
            held_column[slot] = column
            events[total] = column
            return total + new

        return lax.fori_loop(low_of(bounds_ref, u), high_of(bounds_ref, u) + 1, note, total)

    total = lax.fori_loop(0, count, note_unit, jnp.int32(0))
    event_at[count] = total

    def index_copy(n, turn):
        return pltpu.make_async_copy(
            send_ref.at[index_rows(list_ref[n]), :], index[turn], index_sem.at[turn]
        )

    def fetch_first(event, carry):
        fetch(event)
        return carry

    lax.fori_loop(1, jnp.minimum(total, depth), fetch_first, 0)
    for n in range(2):
        pl.when(n < count)(lambda n=n: index_copy(n, n).start())
    for copy in weights:
        copy.wait()
    embed_half[...] = embed_half[...] * jnp.bfloat16(0.5)
    bias_half[...] = bias_half[...] * 0.5

    def one_event(event, carry):
        slot = lax.rem(event, depth)
        pltpu.make_async_copy(
            x_ref.at[:, pl.ds(0, LAT)], points.at[slot], point_sem.at[slot]
        ).wait()
        before = lax.dot_general(
            points[slot], embed_half[...], (((0,), (0,)), ((), ())),
            preferred_element_type=jnp.float32,
        ) + bias_half[...]
        latent = silu_of_double(before)
        base = lax.rem(events[event], SLOTS) * step
        for j in range(parts):
            table[pl.ds(base + j, LAT, stride=parts), :] = latent[:, j * LANES:(j + 1) * LANES]
        pl.when(event + depth < total)(lambda: fetch(event + depth))
        return carry

    def bring(n, turn):
        lax.fori_loop(event_at[n], event_at[n + 1], one_event, 0)
        index_copy(n, turn).wait()

    def gather(turn, half):
        held = (even, odd)[half]
        row = half * (CHUNK // LANES)
        for i in range(CHUNK):
            place = pl.multiple_of(index[turn][row + i // LANES, i % LANES], parts)
            held[pl.ds(parts * i, parts), :] = table[pl.ds(place, parts), :]

    def leave(half, target, start):
        held = (even, odd)[half]
        for j in range(parts):
            target[pl.ds(start, CHUNK), j * LANES:(j + 1) * LANES] = (
                held[pl.ds(j, CHUNK, stride=parts), :].astype(jnp.bfloat16)
            )

    def next_index(n, turn):
        pl.when(n + 2 < count)(lambda: index_copy(n + 2, turn).start())

    return count, list_ref, bring, gather, leave, next_index


def gather_kernel(columns, bounds_ref, send_ref, x_ref, embed_ref, bias_ref, out_ref, *scratch):
    count, _, bring, gather, leave, next_index = point_tools(
        columns, False, bounds_ref, send_ref, x_ref, None, embed_ref, bias_ref, scratch
    )
    spare = out_ref.shape[0] - CHUNK

    def second_half(n):
        place = jnp.where(n > 0, (n - 1) * UNIT + CHUNK, spare)
        return pl.multiple_of(place, CHUNK)

    def one_unit(n, turn):
        bring(n, turn)
        leave(1, out_ref, second_half(n))
        gather(turn, 0)
        leave(0, out_ref, pl.multiple_of(n * UNIT, UNIT))
        gather(turn, 1)
        next_index(n, turn)

    def two_units(m, carry):
        one_unit(2 * m, 0)
        pl.when(2 * m + 1 < count)(lambda: one_unit(2 * m + 1, 1))
        return carry

    lax.fori_loop(0, (count + 1) // 2, two_units, 0)
    pl.when(count > 0)(lambda: leave(1, out_ref, second_half(count)))


def gathered(bounds, send, points, embed_weight, embed_bias):
    channels, width = embed_weight.shape
    columns = points.shape[1] // LAT
    units = send.shape[0] // 8
    most = turn_units(units, lax.axis_size("ch"))
    vmem = pl.BlockSpec(memory_space=pltpu.VMEM)
    smem = pl.BlockSpec(memory_space=pltpu.SMEM)
    hbm = pl.BlockSpec(memory_space=pltpu.HBM)
    return pl.pallas_call(
        functools.partial(gather_kernel, columns),
        in_specs=[smem, hbm, hbm, hbm, hbm],
        out_specs=vmem,
        out_shape=jax.ShapeDtypeStruct((most * UNIT + CHUNK, width), jnp.bfloat16),
        scratch_shapes=point_scratch(units, channels, width),
        compiler_params=pltpu.CompilerParams(vmem_limit_bytes=40 << 20),
        cost_estimate=pl.CostEstimate(
            flops=2 * units * UNIT * channels * width,
            bytes_accessed=units * UNIT * width,
            transcendentals=units * UNIT * width // 2,
        ),
    )(bounds, send, points, embed_weight, embed_bias.reshape(1, -1))


def sum_tools(list_ref, features_ref, recv_ref, sender_all, feature_all, hidden, out_ref):
    nodes, width = out_ref.shape
    parts = width // LANES
    components = features_ref.shape[0]

    def activate(n, turn, rows, terms):
        start = pl.multiple_of(list_ref[n] * UNIT, UNIT)
        mine = slice(turn * UNIT, (turn + 1) * UNIT)
        before = jnp.dot(rows, sender_all[...], preferred_element_type=jnp.float32)
        before += lax.dot_general(
            features_ref[:, pl.ds(start, UNIT)], feature_all[:components, :],
            (((0,), (0,)), ((), ())),
            preferred_element_type=jnp.float32,
        )
        for j in range(parts):
            lanes = slice(j * LANES, (j + 1) * LANES)
            hidden[mine, lanes] = silu_of_double(
                before[:, lanes] + terms[pl.ds(j, UNIT, stride=parts), :]
            ).astype(jnp.bfloat16)

    def add_up(first, turn, number, live=True):
        each = lax.broadcasted_iota(jnp.int32, (nodes, LANES), 0)
        blocks = []
        for n in range(number):
            for b in range(UNIT // LANES):
                ids = recv_ref[pl.ds(list_ref[first + n] * (UNIT // LANES) + b, 1), :]
                ids = ids if live is True else jnp.where(live, ids, -1)
                blocks.append(jnp.where(each == ids, 1.0, 0.0))
        by_node = jnp.concatenate(blocks, axis=1).astype(jnp.bfloat16)
        mine = slice(turn * UNIT, (turn + number) * UNIT)
        out_ref[...] += jnp.dot(by_node, hidden[mine, :], preferred_element_type=jnp.float32)

    return activate, add_up


def edge_kernel(
    columns,
    rows,
    bounds_ref,
    found_ref,
    place_ref,
    recv_ref,
    features_ref,
    *refs,
):
    ways = lax.axis_size("ch")
    pieces = refs[:ways]
    (out_ref, sender_all, recv_terms, feature_all, list_ref, index, receiver_all, even, odd,
     hidden, index_sem) = refs[ways:]
    me = lax.axis_index("ch")
    nodes, width = out_ref.shape
    part = width // ways
    parts = width // LANES
    rings = index.shape[0]
    count = pick_units(bounds_ref, list_ref, list_ref.shape[0] - 1, columns, False)
    activate, add_up = sum_tools(
        list_ref, features_ref, recv_ref, sender_all, feature_all, hidden, out_ref
    )

    def fetch_index(n):
        slot = lax.rem(n, rings)
        return pltpu.make_async_copy(
            place_ref.at[index_rows(list_ref[n]), :], index.at[slot], index_sem.at[slot]
        )

    for n in range(rings - 2):
        pl.when(n < count)(lambda n=n: fetch_index(n).start())
    at = [sum(rows[:n]) for n in range(len(rows) + 1)]
    for j, piece in enumerate(pieces):
        lanes = slice(j * part, (j + 1) * part)
        sender_all[:, lanes] = piece[at[0]:at[1], :] * jnp.bfloat16(0.5)
        receiver_all[:, lanes] = piece[at[1]:at[2], :]
        feature_all[:, lanes] = piece[at[3]:at[4], :] * jnp.bfloat16(0.5)
    components = features_ref.shape[0]
    singles = jnp.concatenate([piece[at[3]:at[4], :] for piece in pieces], axis=1)
    singles = singles.astype(jnp.float32)
    terms = jnp.broadcast_to(
        singles[components:components + 1] + singles[components + 1:components + 2]
        + singles[components + 2:components + 3],
        (nodes, width),
    )
    for j, piece in enumerate(pieces):
        owner = jnp.bitwise_xor(me, j)
        terms += jnp.dot(
            piece[at[2]:at[3], :],
            receiver_all[pl.ds(pl.multiple_of(owner * part, part), part), :],
            preferred_element_type=jnp.float32,
        )
    for j in range(parts):
        recv_terms[pl.ds(j, nodes, stride=parts), :] = (
            0.5 * terms[:, j * LANES:(j + 1) * LANES]
        )
    out_ref[...] = jnp.zeros_like(out_ref)

    def gather(n, held):
        slot = lax.rem(n, rings)
        for i in range(UNIT):
            place = pl.multiple_of(index[slot, i // LANES, i % LANES], parts)
            held[pl.ds(parts * i, parts), :] = recv_terms[pl.ds(place, parts), :]

    def found(n):
        return found_ref[pl.ds(pl.multiple_of(n * UNIT, UNIT), UNIT), :]

    @pl.when(count > 0)
    def _():
        fetch_index(0).wait()
        gather(0, even)

    def pair(m, carry):
        first, second = 2 * m, 2 * m + 1
        after = second + 1 < count
        for n in (first, second):
            pl.when(n + rings - 2 < count)(lambda n=n: fetch_index(n + rings - 2).start())
        fetch_index(second).wait()
        gather(second, odd)
        activate(first, 0, found(first), even)
        pl.when(after)(lambda: fetch_index(second + 1).wait())
        gather(jnp.where(after, second + 1, second), even)
        activate(second, 1, found(second), odd)
        add_up(first, 0, 2)
        return carry

    lax.fori_loop(0, count // 2, pair, 0)

    @pl.when(lax.rem(count, 2) == 1)
    def _():
        activate(count - 1, 0, found(count - 1), even)
        add_up(count - 1, 0, 1)


def first_sums(bounds, found, place, recv, features, pieces, rows, columns, nodes):
    width = found.shape[1]
    units = place.shape[0] // 8
    parts = width // LANES
    vmem = pl.BlockSpec(memory_space=pltpu.VMEM)
    smem = pl.BlockSpec(memory_space=pltpu.SMEM)
    hbm = pl.BlockSpec(memory_space=pltpu.HBM)
    edges = found.shape[0]
    return pl.pallas_call(
        functools.partial(edge_kernel, columns, rows),
        in_specs=[smem, vmem, hbm, vmem, vmem] + [vmem] * len(pieces),
        out_specs=[vmem] * 4,
        out_shape=[
            jax.ShapeDtypeStruct((nodes, width), jnp.float32),
            jax.ShapeDtypeStruct((width, width), jnp.bfloat16),
            jax.ShapeDtypeStruct((nodes * parts, LANES), jnp.float32),
            jax.ShapeDtypeStruct((rows[3], width), jnp.bfloat16),
        ],
        scratch_shapes=[
            pltpu.SMEM((units + 1,), jnp.int32),
            pltpu.SMEM((6, 8, LANES), jnp.int32),
            pltpu.VMEM((width, width), jnp.bfloat16),
            pltpu.VMEM((UNIT * parts, LANES), jnp.float32),
            pltpu.VMEM((UNIT * parts, LANES), jnp.float32),
            pltpu.VMEM((2 * UNIT, width), jnp.bfloat16),
            pltpu.SemaphoreType.DMA((6,)),
        ],
        compiler_params=pltpu.CompilerParams(vmem_limit_bytes=40 << 20),
        cost_estimate=pl.CostEstimate(
            flops=2 * edges * width * (width + nodes),
            bytes_accessed=edges * width,
            transcendentals=edges * width,
        ),
    )(bounds, found, place, recv, features, *pieces)


def later_kernel(
    columns,
    bounds_ref,
    send_ref,
    x_ref,
    halo_ref,
    embed_ref,
    bias_ref,
    place_ref,
    recv_ref,
    features_ref,
    start_ref,
    sender_all,
    recv_terms,
    feature_all,
    out_ref,
    *refs,
):
    scratch = refs[:POINT_SCRATCH]
    (place_even, place_odd, rows_even, rows_odd, terms_even, terms_odd, hidden,
     place_sem) = refs[POINT_SCRATCH:]
    parts = out_ref.shape[1] // LANES
    places, rows, terms = (
        (place_even, place_odd), (rows_even, rows_odd), (terms_even, terms_odd)
    )
    count, list_ref, bring, gather, leave, next_index = point_tools(
        columns, True, bounds_ref, send_ref, x_ref, halo_ref, embed_ref, bias_ref, scratch
    )
    activate, add_up = sum_tools(
        list_ref, features_ref, recv_ref, sender_all, feature_all, hidden, out_ref
    )

    def place_copy(n, turn):
        return pltpu.make_async_copy(
            place_ref.at[index_rows(list_ref[n]), :], places[turn], place_sem.at[turn]
        )

    for n in range(2):
        pl.when(n < count)(lambda n=n: place_copy(n, n).start())
    out_ref[...] = start_ref[...]
    rows_odd[...] = jnp.zeros_like(rows_odd)
    terms_odd[...] = jnp.zeros_like(terms_odd)

    def gather_terms(turn):
        for i in range(UNIT):
            place = pl.multiple_of(places[turn][i // LANES, i % LANES], parts)
            terms[turn][pl.ds(parts * i, parts), :] = recv_terms[pl.ds(place, parts), :]

    def one_unit(n, turn):
        bring(n, turn)
        place_copy(n, turn).wait()
        gather(turn, 0)
        gather(turn, 1)
        before = jnp.maximum(n - 1, 0)
        activate(before, 0, rows[1 - turn][...], terms[1 - turn])
        leave(0, rows[turn], 0)
        leave(1, rows[turn], CHUNK)
        gather_terms(turn)
        add_up(before, 0, 1, n > 0)
        next_index(n, turn)
        pl.when(n + 2 < count)(lambda: place_copy(n + 2, turn).start())

    def two_units(m, carry):
        one_unit(2 * m, 0)
        pl.when(2 * m + 1 < count)(lambda: one_unit(2 * m + 1, 1))
        return carry

    lax.fori_loop(0, (count + 1) // 2, two_units, 0)
    for turn in range(2):
        @pl.when(jnp.logical_and(count > 0, lax.rem(count - 1, 2) == turn))
        def _(turn=turn):
            activate(count - 1, 0, rows[turn][...], terms[turn])
            add_up(count - 1, 0, 1)


def later_sums(bounds, send, points, halo, embed_weight, embed_bias, place, recv, features,
               start, sender_all, recv_terms, feature_all):
    channels, width = embed_weight.shape
    columns = points.shape[1] // LAT
    units = send.shape[0] // 8
    parts = width // LANES
    vmem = pl.BlockSpec(memory_space=pltpu.VMEM)
    smem = pl.BlockSpec(memory_space=pltpu.SMEM)
    hbm = pl.BlockSpec(memory_space=pltpu.HBM)
    return pl.pallas_call(
        functools.partial(later_kernel, columns),
        in_specs=[smem] + [hbm] * 6 + [vmem] * 6,
        out_specs=vmem,
        out_shape=jax.ShapeDtypeStruct(start.shape, jnp.float32),
        scratch_shapes=point_scratch(units, channels, width) + [
            pltpu.SMEM((8, LANES), jnp.int32),
            pltpu.SMEM((8, LANES), jnp.int32),
            pltpu.VMEM((UNIT, width), jnp.bfloat16),
            pltpu.VMEM((UNIT, width), jnp.bfloat16),
            pltpu.VMEM((UNIT * parts, LANES), jnp.float32),
            pltpu.VMEM((UNIT * parts, LANES), jnp.float32),
            pltpu.VMEM((UNIT, width), jnp.bfloat16),
            pltpu.SemaphoreType.DMA((2,)),
        ],
        compiler_params=pltpu.CompilerParams(vmem_limit_bytes=40 << 20),
        cost_estimate=pl.CostEstimate(
            flops=units * UNIT * width * (channels + width),
            bytes_accessed=units * UNIT * width,
            transcendentals=units * UNIT * width,
        ),
    )(bounds, send, points, halo, embed_weight, embed_bias.reshape(1, -1), place, recv,
      features, start, sender_all, recv_terms, feature_all)


def swap_kernel(own_ref, far_ref, own_out, far_out, send, recv):
    beside = across(lax.axis_index("ch"), 1)
    barrier = pltpu.get_barrier_semaphore()
    pl.semaphore_signal(
        barrier, inc=1, device_id={"ch": beside}, device_id_type=pl.DeviceIdType.MESH
    )
    pl.semaphore_wait(barrier, 1)
    copies = [
        pltpu.make_async_remote_copy(
            src_ref=source, dst_ref=target, send_sem=send.at[n], recv_sem=recv.at[n],
            device_id={"ch": beside}, device_id_type=pl.DeviceIdType.MESH,
        )
        for n, (source, target) in enumerate(((own_ref, own_out), (far_ref, far_out)))
    ]
    for copy in copies:
        copy.start()
    for copy in copies:
        copy.wait()


def swapped_beside(own, far):
    vmem = pl.BlockSpec(memory_space=pltpu.VMEM)
    return pl.pallas_call(
        swap_kernel,
        in_specs=[vmem] * 2,
        out_specs=[vmem] * 2,
        out_shape=[jax.ShapeDtypeStruct(own.shape, own.dtype)] * 2,
        scratch_shapes=[pltpu.SemaphoreType.DMA((2,)), pltpu.SemaphoreType.DMA((2,))],
        compiler_params=pltpu.CompilerParams(
            vmem_limit_bytes=8 << 20, collective_id=0, has_side_effects=True
        ),
    )(own, far)


def across(me, bit):
    return me + bit - 2 * bit * lax.rem(me // bit, 2)


def swapped(block, bit, width):
    parts = block.shape[1] // width
    return jnp.concatenate(
        [block[:, (n ^ bit) * width:((n ^ bit) + 1) * width] for n in range(parts)], axis=1
    )


def tail_kernel(
    rows,
    totals_ref,
    recv_ref,
    message_bias_ref,
    *refs,
):
    ch_count = lax.axis_size("ch")
    pieces = refs[:ch_count]
    (out_ref, near, onward, far, normed, give, near_send, near_recv, far_send, far_recv,
     back_send, back_recv, messages) = refs[ch_count:]
    me = lax.axis_index("ch")
    parts, part, width = normed.shape
    beside, opposite = across(me, 1), across(me, 2)
    partners = [beside, opposite, across(opposite, 1)]
    barrier = pltpu.get_barrier_semaphore()
    for partner in partners:
        pl.semaphore_signal(
            barrier, inc=1, device_id={"ch": partner}, device_id_type=pl.DeviceIdType.MESH
        )
    pl.semaphore_wait(barrier, ch_count - 1)

    def copy_to(source, target, send, recv, partner):
        return pltpu.make_async_remote_copy(
            src_ref=source, dst_ref=target, send_sem=send, recv_sem=recv,
            device_id={"ch": partner}, device_id_type=pl.DeviceIdType.MESH,
        )

    half = part // 2
    halves = [pl.ds(n * half, half) for n in range(2)]
    nears = [
        copy_to(
            totals_ref.at[partners[2], some, :], near.at[0, some, :], near_send.at[n],
            near_recv.at[n], beside,
        )
        for n, some in enumerate(halves)
    ]
    nears.append(
        copy_to(totals_ref.at[beside], near.at[1], near_send.at[2], near_recv.at[2], beside)
    )
    for copy in nears:
        copy.start()
    at = [sum(rows[:n]) for n in range(len(rows) + 1)]
    for n in range(parts):
        for j in range(parts):
            first = at[4] + j * width
            messages[n, :, j * width:(j + 1) * width] = pieces[n][first:first + width, :]
    pass_on = []
    for n, some in enumerate(halves):
        nears[n].wait()
        onward[some, :] = (
            totals_ref[opposite, some, :] + swapped(near[0, some, :], 1, width)
        ).astype(onward.dtype)
        pass_on.append(
            copy_to(
                onward.at[some, :], far.at[some, :], far_send.at[n], far_recv.at[n], opposite
            )
        )
        pass_on[n].start()

    def tally(n, counts):
        nodes_here = lax.broadcasted_iota(jnp.int32, (part, LANES), 0) + me * part
        for i in range(8):
            ids = recv_ref[pl.ds(n * 8 + i, 1), :]
            counts = counts + jnp.where(nodes_here == ids, 1.0, 0.0)
        return counts

    counts = lax.fori_loop(
        0, recv_ref.shape[0] // 8, tally, jnp.zeros((part, LANES), jnp.float32)
    )
    aggregated = jnp.sum(counts, axis=1, keepdims=True) * message_bias_ref[...]
    nears[2].wait()
    sums = totals_ref[me] + swapped(near[1], 1, width)
    for copy in pass_on:
        copy.wait()
    sums = sums + swapped(far[...].astype(jnp.float32), 2, width)
    for n in range(parts):
        rest = sums[:, n * width:(n + 1) * width]
        for _ in range(2):
            piece = rest.astype(jnp.bfloat16)
            aggregated += jnp.dot(
                piece, messages[n], preferred_element_type=jnp.float32
            )
            rest = rest - piece.astype(jnp.float32)
    centre = jnp.mean(aggregated, axis=1, keepdims=True)
    spread = jnp.mean(jnp.square(aggregated - centre), axis=1, keepdims=True)
    result = (aggregated - centre) * lax.rsqrt(spread + 1.0)
    for n in range(parts):
        normed[n] = result[:, n * width:(n + 1) * width]
    mine = pl.ds(pl.multiple_of(me * part, part), part)
    returns = []
    for j in (3, 2, 1, 0):
        owner = ([me] + partners)[j]
        small = pieces[j][at[3]:at[4], :].astype(jnp.float32)
        gain = small[7:8] + small[8:9] + small[9:10]
        shift = small[10:11] + small[11:12] + small[12:13]
        latent = pieces[j][pl.ds(at[2] + pl.multiple_of(me * part, part), part), :]
        block = (latent.astype(jnp.float32) + normed[owner] * gain + shift).astype(out_ref.dtype)
        if j == 0:
            out_ref[mine, :] = block
            continue
        give[j - 1] = block
        copy = copy_to(
            give.at[j - 1], out_ref.at[mine, :], back_send.at[j - 1], back_recv.at[j - 1], owner
        )
        copy.start()
        returns.append(copy)
    for copy in returns:
        copy.wait()


def finished(totals, recv, message_bias, pieces, rows, nodes):
    ch_count = lax.axis_size("ch")
    part = nodes // ch_count
    full = totals.shape[1]
    width = full // ch_count
    vmem = pl.BlockSpec(memory_space=pltpu.VMEM)
    return pl.pallas_call(
        functools.partial(tail_kernel, rows),
        in_specs=[vmem] * (3 + ch_count),
        out_specs=vmem,
        out_shape=jax.ShapeDtypeStruct((nodes, width), jnp.bfloat16),
        scratch_shapes=[
            pltpu.VMEM((2, part, full), jnp.float32),
            pltpu.VMEM((part, full), jnp.bfloat16),
            pltpu.VMEM((part, full), jnp.bfloat16),
            pltpu.VMEM((ch_count, part, width), jnp.float32),
            pltpu.VMEM((ch_count - 1, part, width), jnp.bfloat16),
            pltpu.SemaphoreType.DMA((3,)),
            pltpu.SemaphoreType.DMA((3,)),
            pltpu.SemaphoreType.DMA((2,)),
            pltpu.SemaphoreType.DMA((2,)),
            pltpu.SemaphoreType.DMA((ch_count - 1,)),
            pltpu.SemaphoreType.DMA((ch_count - 1,)),
            pltpu.VMEM((ch_count, width, full), jnp.bfloat16),
        ],
        compiler_params=pltpu.CompilerParams(
            vmem_limit_bytes=32 << 20, collective_id=1, has_side_effects=True
        ),
    )(totals.reshape(ch_count, part, full), recv, message_bias.reshape(1, -1), *pieces)


def on_device(
    grid_inputs,
    embed_weight,
    embed_bias,
    mesh_latent,
    edge_features,
    senders,
    receivers,
    sender_weight,
    receiver_weight,
    feature_weight,
    hidden_bias,
    message_weight,
    message_bias,
    norm_gain,
    norm_shift,
):
    lon_count, ch_count = lax.axis_size("lon"), lax.axis_size("ch")
    assert ch_count == 4
    columns = grid_inputs.shape[0] // LAT
    assert columns >= WINDOW
    mesh_nodes = mesh_latent.shape[0]
    width = embed_weight.shape[1]
    assert width == PARTS * LANES
    edges = senders.shape[0]
    unit = UNIT
    assert edges % unit == 0 and unit == 2 * CHUNK
    points = grid_inputs.T

    edge_columns = cut_columns(points)
    packed, send, recv, place, bounds = prepared(
        columns, senders, receivers, sender_weight, receiver_weight, mesh_latent,
        feature_weight, hidden_bias, norm_gain, norm_shift, message_weight,
    )
    rows = (width, width, mesh_nodes, 16)
    hops = []
    for i in range(lon_count):
        hops.append((i * ch_count, (i + 1) % lon_count * ch_count))
        hops.append(
            (i * ch_count + ch_count - 1, (i - 1) % lon_count * ch_count + ch_count - 1)
        )
    halo = lax.ppermute(edge_columns, ("lon", "ch"), hops)

    opposite = lax.ppermute(packed, "ch", [(i, i ^ 2) for i in range(ch_count)])
    beside, diagonal = swapped_beside(packed, opposite)
    pieces = [packed, beside, opposite, diagonal]

    found = gathered(bounds, send, points, embed_weight, embed_bias)
    totals, *prepared_weights = first_sums(
        bounds, found, place, recv, edge_features, pieces, rows, columns, mesh_nodes
    )
    totals = later_sums(
        bounds, send, points, halo, embed_weight, embed_bias, place, recv, edge_features,
        totals, *prepared_weights,
    )
    return finished(
        totals, recv, message_bias, pieces, rows, mesh_nodes
    )


def solution(mesh):
    return jax.shard_map(
        on_device,
        mesh=mesh,
        in_specs=(
            P("lon", None),
            P(),
            P(),
            P("lon", "ch"),
            P(None, "lon"),
            P("lon"),
            P("lon"),
            P(None, "ch"),
            P(None, "ch"),
            P(None, "ch"),
            P("ch"),
            P("ch", None),
            P(),
            P("ch"),
            P("ch"),
        ),
        out_specs=P("lon", "ch"),
        check_vma=False,
    )
```
